128 devices in a mesh: data: 1, col: 16 (over z, y), row: 8 (over x, core).
Axes of the slice: x: 4, y: 4, z: 4, core: 2. Of those that a mesh axis runs over, the one named last changes fastest.
Arguments:
- pair_rep: bfloat16 [768, 768, 128], P(('data', 'row'), 'col')
- res_mask: int32 [768], P('data')
- ln_gamma: float32 [128], replicated
- ln_beta: float32 [128], replicated
- w_q: bfloat16 [128, 128], replicated
- w_k: bfloat16 [128, 128], replicated
- w_v: bfloat16 [128, 128], replicated
- w_b: bfloat16 [128, 4], replicated
- w_g: bfloat16 [128, 128], replicated
- w_o: bfloat16 [128, 128], replicated
Outputs:
- output: bfloat16 [768, 768, 128], P(('data', 'row'), 'col')
All inputs are finite; a program needn't handle non-finite values.
Results may differ from the reference program's by a relative error of at most 0.00639987.
Values are sent between devices in bfloat16 or wider.
A program may use at most 1 GiB of HBM per device.

```python
import math
import jax
import jax.numpy as jnp
from jax import lax

N = 768
C_Z = 128
HEADS = 4
HEAD = 32

PROJ = HEADS * HEAD
Q_SCALE = 1.0 / math.sqrt(HEAD)
LN_EPS = 1e-5
MASK_FILL = -1e9
OUT_GAIN = 0.35 * math.sqrt(N / PROJ)


def setup_inputs(seed: int = 0, part: int = 0) -> dict:
    base_key = jax.random.key(seed)
    part_key = jax.random.fold_in(base_key, part)
    key_pair, key_len = jax.random.split(part_key, 2)
    pair_rep = jax.random.normal(key_pair, (N, N, C_Z), jnp.float32).astype(jnp.bfloat16)
    pad_len = jax.random.randint(key_len, (), N // 16, N // 4 + 1)
    res_mask = (jnp.arange(N) < N - pad_len).astype(jnp.int32)
    weight_keys = jax.random.split(base_key, 8)
    in_scale = 1.0 / math.sqrt(C_Z)
    ln_gamma = jax.random.uniform(weight_keys[0], (C_Z,), jnp.float32, 0.5, 1.5)
    ln_beta = 0.1 * jax.random.normal(weight_keys[1], (C_Z,), jnp.float32)
    w_q = (in_scale * jax.random.normal(weight_keys[2], (C_Z, PROJ), jnp.float32)).astype(jnp.bfloat16)
    w_k = (in_scale * jax.random.normal(weight_keys[3], (C_Z, PROJ), jnp.float32)).astype(jnp.bfloat16)
    w_v = (in_scale * jax.random.normal(weight_keys[4], (C_Z, PROJ), jnp.float32)).astype(jnp.bfloat16)
    w_b = (in_scale * jax.random.normal(weight_keys[5], (C_Z, HEADS), jnp.float32)).astype(jnp.bfloat16)
    w_g = (in_scale * jax.random.normal(weight_keys[6], (C_Z, PROJ), jnp.float32)).astype(jnp.bfloat16)
    w_o = (OUT_GAIN * jax.random.normal(weight_keys[7], (PROJ, C_Z), jnp.float32)).astype(jnp.bfloat16)
    return {'pair_rep': pair_rep, 'res_mask': res_mask, 'ln_gamma': ln_gamma, 'ln_beta': ln_beta, 'w_q': w_q, 'w_k': w_k, 'w_v': w_v, 'w_b': w_b, 'w_g': w_g, 'w_o': w_o}


def reference(pair_rep, res_mask, ln_gamma, ln_beta, w_q, w_k, w_v, w_b, w_g, w_o):
    pair_f32 = pair_rep.astype(jnp.float32)
    mean = jnp.mean(pair_f32, axis=-1, keepdims=True)
    centred = pair_f32 - mean
    variance = jnp.mean(centred * centred, axis=-1, keepdims=True)
    normed = (centred * lax.rsqrt(variance + LN_EPS) * ln_gamma + ln_beta).astype(jnp.bfloat16)
    bias = jnp.dot(normed.reshape(N * N, C_Z), w_b, preferred_element_type=jnp.float32).astype(jnp.bfloat16).reshape(N, N, HEADS)
    key_fill = jnp.where(res_mask > 0, 0.0, MASK_FILL).astype(jnp.float32)
    bias_ik = jnp.transpose(bias, (1, 0, 2)).astype(jnp.float32) + key_fill[None, :, None]

    def one_column(col_args):
        a_col, z_col = col_args
        query = (jnp.dot(a_col, w_q, preferred_element_type=jnp.float32) * Q_SCALE).astype(jnp.bfloat16).reshape(N, HEADS, HEAD)
        keys = jnp.dot(a_col, w_k, preferred_element_type=jnp.float32).astype(jnp.bfloat16).reshape(N, HEADS, HEAD)
        values = jnp.dot(a_col, w_v, preferred_element_type=jnp.float32).astype(jnp.bfloat16).reshape(N, HEADS, HEAD)
        gate = jax.nn.sigmoid(jnp.dot(a_col, w_g, preferred_element_type=jnp.float32))
        logits = jnp.einsum('ihd,khd->ikh', query.astype(jnp.float32), keys.astype(jnp.float32)) + bias_ik
        attn_prob = jax.nn.softmax(logits, axis=1)
        attended = jnp.einsum('ikh,khd->ihd', attn_prob, values.astype(jnp.float32)).reshape(N, PROJ)
        gated = (gate * attended).astype(jnp.bfloat16)
        return (z_col.astype(jnp.float32) + jnp.dot(gated, w_o, preferred_element_type=jnp.float32)).astype(jnp.bfloat16)

    out_cols = lax.map(one_column, (jnp.transpose(normed, (1, 0, 2)), jnp.transpose(pair_rep, (1, 0, 2))))
    return jnp.transpose(out_cols, (1, 0, 2))
```

```python
import math
import jax
import jax.numpy as jnp
from jax import lax
from jax.experimental import pallas as pl
from jax.experimental.pallas import tpu as pltpu
from jax.sharding import PartitionSpec as P

LN_EPS = 1e-5
MASK_FILL = -1e9
LOG2E = math.log2(math.e)
NT = (((1,), (1,)), ((), ()))


def layer_norm(z, gamma, beta):
    mean = jnp.mean(z, axis=-1, keepdims=True)
    centred = z - mean
    variance = jnp.mean(centred * centred, axis=-1, keepdims=True)
    return (centred * lax.rsqrt(variance + LN_EPS) * gamma + beta).astype(jnp.bfloat16)


def attend_kernel(z_ref, bias_ref, mask_ref, gamma_ref, beta_ref, wq_ref, wk_ref, wv_ref, wg_ref, wo_ref, out_ref,
                  a_s, k_s, vt_s, qt_s, bias_s, fill_s, wt_s, s_a, s_b, o_s):
    f32, bf16 = jnp.float32, jnp.bfloat16
    rows, cols, block, chan = z_ref.shape
    n = rows * block
    heads = bias_ref.shape[0]
    hd = chan // heads
    tile = 256
    nt = n // tile

    for idx, w in enumerate((wq_ref, wv_ref, wg_ref, wo_ref)):
        wt_s[idx] = w[...].astype(f32).T.astype(bf16)
    fill = jnp.where(mask_ref[...] > 0, 0.0, MASK_FILL).astype(f32)
    for t in range(n // 128):
        fill_s[pl.ds(t * 128, 128), :] = jnp.broadcast_to(fill[:, t * 128:(t + 1) * 128], (128, 128)).T

    eye = (lax.broadcasted_iota(jnp.int32, (tile, tile), 0) == lax.broadcasted_iota(jnp.int32, (tile, tile), 1)).astype(f32).astype(bf16)

    @pl.loop(0, heads * nt)
    def _(step):
        h = step // nt
        it = step % nt
        for kt in range(nt):
            part = bias_ref[h, pl.ds(pl.multiple_of(it * tile, tile), tile), pl.ds(kt * tile, tile)]
            out = lax.dot_general(eye, part, NT, preferred_element_type=f32)
            fl = fill_s[pl.ds(kt * tile, tile), :]
            bias_s[h, it, pl.ds(kt * tile, tile), :] = out + jnp.concatenate([fl, fl], axis=1)

    @pl.loop(0, cols)
    def _(j):
        z = z_ref[:, j].astype(f32).reshape(n, chan)
        a = layer_norm(z, gamma_ref[...], beta_ref[...])
        a_s[j] = a
        k_s[j] = jnp.dot(a, wk_ref[...], preferred_element_type=f32).astype(bf16)
        vt_s[j] = lax.dot_general(wt_s[1], a, NT, preferred_element_type=f32).astype(bf16)
        qt = (lax.dot_general(wt_s[0], a, NT, preferred_element_type=f32) * (1.0 / math.sqrt(hd))).astype(bf16)
        zero = jnp.zeros((hd, n), bf16)
        for h in range(heads):
            qt_s[j, h] = jnp.concatenate([qt[h * hd:(h + 1) * hd] if g == h else zero for g in range(heads)], axis=0)

    def logits(j, h, it, s_ref):
        qt = qt_s[j, h, :, pl.ds(pl.multiple_of(it * tile, tile), tile)]
        s_ref[...] = jnp.dot(k_s[j], qt, preferred_element_type=f32) + bias_s[h, it]

    def finish_tile(j, h, it, s_ref):
        s = s_ref[...]
        top = jnp.max(s, axis=0, keepdims=True)
        p = jnp.exp2((s - top) * LOG2E)
        total = jnp.sum(p, axis=0, keepdims=True)
        vt = vt_s[j, pl.ds(pl.multiple_of(h * hd, hd), hd), :]
        o = jnp.dot(vt, p.astype(bf16), preferred_element_type=f32)
        o_s[j, pl.ds(pl.multiple_of(h * hd, hd), hd), pl.ds(pl.multiple_of(it * tile, tile), tile)] = o / total

    def coords(step):
        return step // (heads * nt), (step // nt) % heads, step % nt

    steps = cols * heads * nt
    logits(0, 0, 0, s_a)

    @pl.loop(0, steps // 2)
    def _(u):
        logits(*coords(2 * u + 1), s_b)
        finish_tile(*coords(2 * u), s_a)
        logits(*coords(jnp.minimum(2 * u + 2, steps - 1)), s_a)
        finish_tile(*coords(2 * u + 1), s_b)

    @pl.loop(0, cols)
    def _(j):
        gate = jax.nn.sigmoid(lax.dot_general(wt_s[2], a_s[j], NT, preferred_element_type=f32))
        gated = (gate * o_s[j]).astype(bf16)
        update = jnp.dot(wt_s[3], gated, preferred_element_type=f32)
        res = z_ref[:, j].astype(f32).reshape(n, chan) + update.T
        out_ref[:, j] = res.astype(bf16).reshape(rows, block, chan)


def solution(mesh):
    rows = mesh.shape['row']

    def body(pair_tile, res_mask, ln_gamma, ln_beta, w_q, w_k, w_v, w_b, w_g, w_o):
        block, width, chan = pair_tile.shape
        heads = w_b.shape[1]
        n = block * rows
        cols = width // rows
        bf16, f32 = jnp.bfloat16, jnp.float32
        normed = layer_norm(pair_tile.astype(f32), ln_gamma, ln_beta)
        bias_tile = jnp.einsum('kic,ch->hik', normed, w_b, preferred_element_type=f32).astype(bf16)
        bias = lax.all_gather(bias_tile, 'col', axis=1, tiled=True)
        bias = lax.all_gather(bias, 'row', axis=2, tiled=True)
        zt = jnp.transpose(pair_tile, (1, 0, 2)).reshape(rows, cols, block, chan)
        zr = lax.all_to_all(zt, 'row', 0, 0, tiled=True)
        V = lambda *s, dt=bf16: pltpu.VMEM(s, dt)
        out = pl.pallas_call(
            attend_kernel,
            out_shape=jax.ShapeDtypeStruct((rows, cols, block, chan), bf16),
            in_specs=[pl.BlockSpec(memory_space=pltpu.VMEM)] * 10,
            out_specs=pl.BlockSpec(memory_space=pltpu.VMEM),
            scratch_shapes=[V(cols, n, chan), V(cols, n, chan), V(cols, chan, n), V(cols, heads, chan, n),
                            V(heads, n // 256, n, 256, dt=f32), V(n, 128, dt=f32), V(4, chan, chan),
                            V(n, 256, dt=f32), V(n, 256, dt=f32), V(cols, chan, n, dt=f32)],
            compiler_params=pltpu.CompilerParams(vmem_limit_bytes=60000 * 1024),
            name='attend',
        )(zr, bias, res_mask.reshape(1, n), ln_gamma.reshape(1, chan), ln_beta.reshape(1, chan), w_q, w_k, w_v, w_g, w_o)
        back = lax.all_to_all(out, 'row', 0, 0, tiled=True)
        return jnp.transpose(back.reshape(width, block, chan), (1, 0, 2))

    tile_spec = P(('data', 'row'), 'col', None)
    return jax.shard_map(body, mesh=mesh, in_specs=(tile_spec, P('data'), P(), P(), P(), P(), P(), P(), P(), P()), out_specs=tile_spec, check_vma=False)
```

```python
import math
import jax
import jax.numpy as jnp
from jax import lax
from jax.experimental import pallas as pl
from jax.experimental.pallas import tpu as pltpu
from jax.sharding import PartitionSpec as P

LN_EPS = 1e-5
MASK_FILL = -1e9
LOG2E = math.log2(math.e)
NT = (((1,), (1,)), ((), ()))
MESH = pl.DeviceIdType.MESH
TILE = 256
RING = 4


def layer_norm(z, gamma, beta):
    mean = jnp.mean(z, axis=-1, keepdims=True)
    centred = z - mean
    variance = jnp.mean(centred * centred, axis=-1, keepdims=True)
    return (centred * lax.rsqrt(variance + LN_EPS) * gamma + beta).astype(jnp.bfloat16)


def triangle_kernel(z_ref, mask_ref, gamma_ref, beta_ref, wq_ref, wk_ref, wv_ref, wb_ref, wg_ref, wo_ref, out_ref,
                    zr_s, wb_s, bst_s, bt_s, gb_s, bias_s, biasf_s, fill_s, wt_s, a_s, k_s, vt_s, qt_s, s_a, s_b, o_s, res_s,
                    g_send, g_recv, z_send, z_recv, p_send, p_recv, d_send, d_recv, o_send, o_recv, loc_sem):
    f32, bf16 = jnp.float32, jnp.bfloat16
    data, col, row = lax.axis_index('data'), lax.axis_index('col'), lax.axis_index('row')
    rows, cols, block, chan = zr_s.shape
    width = rows * cols
    n = rows * block
    heads = qt_s.shape[1]
    hd = chan // heads
    nt = n // TILE
    core = row % 2
    zc, yc = col // RING, col % RING

    def dev(c, r):
        return (data, c, r)

    def row_peer(d):
        return dev(col, (row + d) % rows)

    def plane_peer(along_y, d):
        if along_y:
            return dev(zc * RING + (yc + d) % RING, row)
        return dev((zc + d) % RING * RING + yc, row)

    barrier = pltpu.get_barrier_semaphore()
    for d in range(1, rows):
        pl.semaphore_signal(barrier, inc=1, device_id=row_peer(d), device_id_type=MESH)
    for along_y in (True, False):
        for d in range(1, RING):
            pl.semaphore_signal(barrier, inc=1, device_id=plane_peer(along_y, d), device_id_type=MESH)

    gamma, beta = gamma_ref[...], beta_ref[...]
    wb_s[...] = jnp.zeros_like(wb_s)
    wb_s[:, :heads] = wb_ref[...].astype(f32)
    wbt = wb_s[...].T[:8].astype(bf16)
    bst_s[...] = jnp.zeros_like(bst_s)
    group = 8

    @pl.loop(0, width // group)
    def _(g):
        a = layer_norm(z_ref[pl.ds(g * group, group)].astype(f32).reshape(group * block, chan), gamma, beta)
        for t in range(group):
            b = lax.dot_general(wbt, a[t * block:(t + 1) * block], NT, preferred_element_type=f32)
            for h in range(heads):
                bst_s[h, pl.ds(g * group + t, 1), :block] = b[h:h + 1]

    for h in range(heads):
        bt_s[h // 2, h % 2] = bst_s[h].astype(bf16)

    pl.semaphore_wait(barrier, rows - 1 + 2 * (RING - 1))

    def g_copy(d):
        peer = (row + d) % rows
        return pltpu.make_async_remote_copy(src_ref=bt_s.at[peer % 2], dst_ref=gb_s.at[d], send_sem=g_send.at[d], recv_sem=g_recv.at[d],
                                            device_id=dev(col, peer), device_id_type=MESH)

    def z_copy(d, ck):
        peer = (row + d) % rows
        return pltpu.make_async_remote_copy(src_ref=z_ref.at[pl.ds(peer * cols + 2 * ck, 2)], dst_ref=zr_s.at[row, pl.ds(2 * ck, 2)],
                                            send_sem=z_send.at[d, ck], recv_sem=z_recv.at[d, ck], device_id=dev(col, peer), device_id_type=MESH)

    for d in range(1, rows):
        g_copy(d).start()
    for ck in range(cols // 2):
        for d in range(1, rows):
            z_copy(d, ck).start()
    own_z = pltpu.make_async_copy(z_ref.at[pl.ds(row * cols, cols)], zr_s.at[row], loc_sem.at[0])
    own_z.start()

    for idx, w in enumerate((wq_ref, wv_ref, wg_ref, wo_ref)):
        wt_s[idx] = w[...].astype(f32).T.astype(bf16)
    fill = jnp.where(mask_ref[...] > 0, 0.0, MASK_FILL).astype(f32)
    for t in range(n // 128):
        fill_s[pl.ds(t * 128, 128), :] = jnp.broadcast_to(fill[:, t * 128:(t + 1) * 128], (128, 128)).T
    gb_s[0] = bt_s[core]

    for d in range(1, rows):
        g_copy(d).wait_recv()
    lane = lax.broadcasted_iota(jnp.int32, (width, 128), 1)
    for hh in range(2):
        for half in range(2):
            for t in range(3):
                lo = half * 4 + t
                first = gb_s[(row - lo + rows) % rows, hh].astype(f32)
                second = gb_s[(row - lo - 1 + rows) % rows, hh].astype(f32)
                cut = block - 32 * t
                piece = jnp.where(lane < cut, pltpu.roll(first, (128 - 32 * t) % 128, 1), pltpu.roll(second, cut, 1))
                bias_s[2 * core + hh, half, zc, yc, :, t * 128:(t + 1) * 128] = piece.astype(bf16)

    def plane_copy(w, half, first, origin, d):
        along_y = (half == 0) == first
        oz, oy = (zc, (yc + origin) % RING) if half == 0 else ((zc + origin) % RING, yc)
        blk = bias_s.at[2 * core + w, half, oz, oy]
        k = 0 if first else 1 + origin
        return pltpu.make_async_remote_copy(src_ref=blk, dst_ref=blk, send_sem=p_send.at[w, half, k, d], recv_sem=p_recv.at[w, half, k, d],
                                            device_id=plane_peer(along_y, d), device_id_type=MESH)

    def plane_open(w):
        for half in range(2):
            for d in (1, 3, 2):
                plane_copy(w, half, True, 0, d).start()
        for half in range(2):
            for d in (1, 3, 2):
                plane_copy(w, half, False, 0, d).start()

    def plane_forward(w):
        for d in (1, 3, 2):
            for half in range(2):
                plane_copy(w, half, True, 0, d).wait_recv()
                for e in (1, 3, 2):
                    plane_copy(w, half, False, RING - d, e).start()

    def plane_close(w):
        for half in range(2):
            for origin in (0, 3, 1, 2):
                for d in (1, 3, 2):
                    plane_copy(w, half, False, origin, d).wait_recv()

    def pair_copy(w, half):
        blk = bias_s.at[2 * core + w, half]
        return pltpu.make_async_remote_copy(src_ref=blk, dst_ref=blk, send_sem=d_send.at[w, half], recv_sem=d_recv.at[w, half],
                                            device_id=dev(col, row + 1 - 2 * core), device_id_type=MESH)

    def project(ck):
        for d in range(1, rows):
            z_copy(d, ck).wait_recv()

        @pl.loop(0, 2)
        def _(jj):
            j = 2 * ck + jj
            a = layer_norm(zr_s[:, j].astype(f32).reshape(n, chan), gamma, beta)
            a_s[j] = a
            k_s[j] = jnp.dot(a, wk_ref[...], preferred_element_type=f32).astype(bf16)
            vt_s[j] = lax.dot_general(wt_s[1], a, NT, preferred_element_type=f32).astype(bf16)
            qt = (lax.dot_general(wt_s[0], a, NT, preferred_element_type=f32) * (1.0 / math.sqrt(hd))).astype(bf16)
            zero = jnp.zeros((hd, n), bf16)
            for h in range(heads):
                qt_s[j, h] = jnp.concatenate([qt[h * hd:(h + 1) * hd] if g == h else zero for g in range(heads)], axis=0)

    eye = (lax.broadcasted_iota(jnp.int32, (128, 128), 0) == lax.broadcasted_iota(jnp.int32, (128, 128), 1)).astype(f32).astype(bf16)

    def expand_bias(w):
        @pl.loop(0, 2)
        def _(hh):
            h = 2 * hh + w
            for half in range(2):
                val = bias_s[h, half].reshape(n, n // 2)
                for it in range(nt):
                    for kt in range(3):
                        lo = half * (n // 2) + kt * 128
                        out = lax.dot_general(eye, val[it * TILE:(it + 1) * TILE, kt * 128:(kt + 1) * 128], NT, preferred_element_type=f32)
                        fl = fill_s[pl.ds(lo, 128), :]
                        biasf_s[h, it, pl.ds(lo, 128), :] = out + jnp.concatenate([fl, fl], axis=1)

    per_col = 2 * nt

    def coords(w, step):
        return step // per_col, 2 * (step // nt % 2) + w, step % nt

    def logits(w, step, s_ref):
        j, h, it = coords(w, step)
        qt = qt_s[j, h, :, pl.ds(pl.multiple_of(it * TILE, TILE), TILE)]
        s_ref[...] = jnp.dot(k_s[j], qt, preferred_element_type=f32) + biasf_s[h, it]

    def finish_tile(w, step, s_ref):
        j, h, it = coords(w, step)
        s = s_ref[...]
        top = jnp.max(s, axis=0, keepdims=True)
        p = jnp.exp2((s - top) * LOG2E)
        total = jnp.sum(p, axis=0, keepdims=True)
        rows_h = pl.ds(pl.multiple_of(h * hd, hd), hd)
        o = jnp.dot(vt_s[j, rows_h, :], p.astype(bf16), preferred_element_type=f32)
        o_s[j, rows_h, pl.ds(pl.multiple_of(it * TILE, TILE), TILE)] = o / total

    def out_copy(j, d):
        peer = (row + d) % rows
        return pltpu.make_async_remote_copy(src_ref=res_s.at[j, peer], dst_ref=out_ref.at[row * cols + j], send_sem=o_send.at[j, d],
                                            recv_sem=o_recv.at[j, d], device_id=dev(col, peer), device_id_type=MESH)

    def own_out(j):
        return pltpu.make_async_copy(res_s.at[j, row], out_ref.at[row * cols + j], o_send.at[j, 0])

    def finish_column(j):
        gate = jax.nn.sigmoid(lax.dot_general(wt_s[2], a_s[j], NT, preferred_element_type=f32))
        gated = (gate * o_s[j]).astype(bf16)
        update = jnp.dot(wt_s[3], gated, preferred_element_type=f32)
        res = zr_s[:, j].astype(f32).reshape(n, chan) + update.T
        res_s[j] = res.astype(bf16).reshape(rows, block, chan)
        for d in range(1, rows):
            out_copy(j, d).start()
        own_out(j).start()

    def attend(w, j_lo, j_hi, last):
        @pl.loop(j_lo, j_hi)
        def _(j):
            @pl.loop(0, nt)
            def _(u):
                step = j * per_col + 2 * u
                logits(w, step + 1, s_b)
                finish_tile(w, step, s_a)
                logits(w, jnp.minimum(step + 2, cols * per_col - 1), s_a)
                finish_tile(w, step + 1, s_b)
            if last:
                finish_column(j)

    plane_open(0)
    plane_forward(0)
    plane_open(1)
    own_z.wait()
    project(0)
    plane_forward(1)
    project(1)
    plane_close(0)
    for half in range(2):
        pair_copy(0, half).start()
    project(2)
    for half in range(2):
        pair_copy(0, half).wait_recv()
    expand_bias(0)
    logits(0, 0, s_a)
    attend(0, 0, cols // 2, False)
    plane_close(1)
    for half in range(2):
        pair_copy(1, half).start()
    attend(0, cols // 2, cols, False)
    for half in range(2):
        pair_copy(1, half).wait_recv()
    expand_bias(1)
    logits(1, 0, s_a)
    attend(1, 0, cols, True)

    for d in range(1, rows):
        g_copy(d).wait_send()
        for ck in range(cols // 2):
            z_copy(d, ck).wait_send()
    for w in range(2):
        for half in range(2):
            pair_copy(w, half).wait_send()
            for d in range(1, RING):
                plane_copy(w, half, True, 0, d).wait_send()
                for origin in range(RING):
                    plane_copy(w, half, False, origin, d).wait_send()

    @pl.loop(0, cols)
    def _(j):
        for d in range(1, rows):
            out_copy(j, d).wait()
        own_out(j).wait()


def solution(mesh):
    rows = mesh.shape['row']

    def body(pair_tile, res_mask, ln_gamma, ln_beta, w_q, w_k, w_v, w_b, w_g, w_o):
        block, width, chan = pair_tile.shape
        heads = w_b.shape[1]
        n = block * rows
        cols = width // rows
        bf16, f32 = jnp.bfloat16, jnp.float32
        zt = jnp.transpose(pair_tile, (1, 0, 2))
        V = lambda *s, dt=bf16: pltpu.VMEM(s, dt)
        D = lambda *s: pltpu.SemaphoreType.DMA(s)
        out = pl.pallas_call(
            triangle_kernel,
            out_shape=jax.ShapeDtypeStruct((width, block, chan), bf16),
            in_specs=[pl.BlockSpec(memory_space=pltpu.VMEM)] * 10,
            out_specs=pl.BlockSpec(memory_space=pl.ANY),
            scratch_shapes=[V(rows, cols, block, chan), V(chan, 128, dt=f32), V(heads, width, 128, dt=f32), V(2, 2, width, 128),
                            V(rows, 2, width, 128), V(heads, 2, RING, RING, width, n // 2), V(heads, n // TILE, n, TILE, dt=f32),
                            V(n, 128, dt=f32), V(4, chan, chan), V(cols, n, chan), V(cols, n, chan), V(cols, chan, n),
                            V(cols, heads, chan, n), V(n, TILE, dt=f32), V(n, TILE, dt=f32), V(cols, chan, n, dt=f32),
                            V(cols, rows, block, chan),
                            D(rows), D(rows), D(rows, cols // 2), D(rows, cols // 2), D(2, 2, RING + 1, RING), D(2, 2, RING + 1, RING),
                            D(2, 2), D(2, 2), D(cols, rows), D(cols, rows), D(1)],
            compiler_params=pltpu.CompilerParams(vmem_limit_bytes=60000 * 1024, collective_id=0, has_side_effects=True),
            name='triangle',
        )(zt, res_mask.reshape(1, n), ln_gamma.reshape(1, chan), ln_beta.reshape(1, chan), w_q, w_k, w_v, w_b, w_g, w_o)
        return jnp.transpose(out, (1, 0, 2))

    tile_spec = P(('data', 'row'), 'col', None)
    return jax.shard_map(body, mesh=mesh, in_specs=(tile_spec, P('data'), P(), P(), P(), P(), P(), P(), P(), P()), out_specs=tile_spec, check_vma=False)
```

```python
import math
import jax
import jax.numpy as jnp
from jax import lax
from jax.experimental import pallas as pl
from jax.experimental.pallas import tpu as pltpu
from jax.sharding import PartitionSpec as P

LN_EPS = 1e-5
MASK_FILL = -1e9
LOG2E = math.log2(math.e)
NT = (((1,), (1,)), ((), ()))
MESH = pl.DeviceIdType.MESH
TILE = 256
RING = 4


def layer_norm(z, gamma, beta):
    mean = jnp.mean(z, axis=-1, keepdims=True)
    centred = z - mean
    variance = jnp.mean(centred * centred, axis=-1, keepdims=True)
    return (centred * lax.rsqrt(variance + LN_EPS) * gamma + beta).astype(jnp.bfloat16)


def triangle_kernel(z_ref, mask_ref, gamma_ref, beta_ref, wq_ref, wk_ref, wv_ref, wb_ref, wg_ref, wo_ref, out_ref,
                    zr_s, bst_s, bt_s, gb_s, bias_s, biasf_s, wt_s, a_s, k_s, vt_s, qt_s, s_a, s_b, m_a, m_b, o_s, res_s,
                    g_send, g_recv, z_send, z_recv, p_send, p_recv, d_send, d_recv, o_send, o_recv, loc_sem):
    f32, bf16 = jnp.float32, jnp.bfloat16
    data, col, row = lax.axis_index('data'), lax.axis_index('col'), lax.axis_index('row')
    rows, cols, chan = zr_s.shape[0], zr_s.shape[1], zr_s.shape[-1]
    width = rows * cols
    block = z_ref.shape[1] * z_ref.shape[2] * z_ref.shape[3]
    n = rows * block
    heads = wb_ref.shape[0]
    hd = chan // heads
    nt = n // TILE
    sub = width // nt
    core = row % 2
    zc, yc = col // RING, col % RING

    def dev(c, r):
        return (data, c, r)

    def row_peer(d):
        return dev(col, (row + d) % rows)

    def plane_peer(along_y, d):
        if along_y:
            return dev(zc * RING + (yc + d) % RING, row)
        return dev((zc + d) % RING * RING + yc, row)

    barrier = pltpu.get_barrier_semaphore()
    for d in range(1, rows):
        pl.semaphore_signal(barrier, inc=1, device_id=row_peer(d), device_id_type=MESH)
    for along_y in (True, False):
        for d in range(1, RING):
            pl.semaphore_signal(barrier, inc=1, device_id=plane_peer(along_y, d), device_id_type=MESH)

    gamma, beta = gamma_ref[...], beta_ref[...]
    wbt = wb_ref[...]
    bst_s[...] = jnp.zeros_like(bst_s)
    group = 8

    @pl.loop(0, width // group)
    def _(g):
        a = layer_norm(z_ref[pl.ds(g * group, group)].astype(f32).reshape(group * block, chan), gamma, beta)
        for t in range(group):
            b = lax.dot_general(wbt, a[t * block:(t + 1) * block], NT, preferred_element_type=f32)
            for h in range(heads):
                bst_s[h, pl.ds(g * group + t, 1), :block] = b[h:h + 1]

    for h in range(heads):
        bt_s[h // 2, h % 2] = bst_s[h].astype(bf16)

    pl.semaphore_wait(barrier, rows - 1 + 2 * (RING - 1))

    def g_copy(d):
        peer = (row + d) % rows
        return pltpu.make_async_remote_copy(src_ref=bt_s.at[peer % 2], dst_ref=gb_s.at[d], send_sem=g_send.at[d], recv_sem=g_recv.at[d],
                                            device_id=dev(col, peer), device_id_type=MESH)

    def z_copy(d, ck):
        peer = (row + d) % rows
        return pltpu.make_async_remote_copy(src_ref=z_ref.at[pl.ds(peer * cols + 2 * ck, 2)], dst_ref=zr_s.at[row, pl.ds(2 * ck, 2)],
                                            send_sem=z_send.at[d, ck], recv_sem=z_recv.at[d, ck], device_id=dev(col, peer), device_id_type=MESH)

    for d in range(1, rows):
        g_copy(d).start()
    for ck in range(cols // 2):
        for d in range(1, rows):
            z_copy(d, ck).start()
    own_z = pltpu.make_async_copy(z_ref.at[pl.ds(row * cols, cols)], zr_s.at[row], loc_sem.at[0])
    own_z.start()

    for idx, w in enumerate((wq_ref, wv_ref, wg_ref, wo_ref)):
        wt_s[idx] = w[...].astype(f32).T.astype(bf16)
    kept = jnp.sum(mask_ref[...].reshape(1, n), axis=1, keepdims=True)
    gb_s[0] = bt_s[core]

    for d in range(1, rows):
        g_copy(d).wait_recv()
    lane = lax.broadcasted_iota(jnp.int32, (width, 128), 1)
    for hh in range(2):
        for half in range(2):
            for t in range(3):
                lo = half * 4 + t
                first = gb_s[(row - lo + rows) % rows, hh].astype(f32)
                second = gb_s[(row - lo - 1 + rows) % rows, hh].astype(f32)
                cut = block - 32 * t
                piece = jnp.where(lane < cut, pltpu.roll(first, (128 - 32 * t) % 128, 1), pltpu.roll(second, cut, 1))
                for it in range(nt):
                    bias_s[core, it, half, zc, yc, hh, :, t * 128:(t + 1) * 128] = piece[it * sub:(it + 1) * sub].astype(bf16)

    def plane_copy(w, half, first, origin, d):
        along_y = (half == 0) == first
        oz, oy = (zc, (yc + origin) % RING) if half == 0 else ((zc + origin) % RING, yc)
        blk = bias_s.at[core, w, half, oz, oy]
        k = 0 if first else 1 + origin
        return pltpu.make_async_remote_copy(src_ref=blk, dst_ref=blk, send_sem=p_send.at[w, half, k, d], recv_sem=p_recv.at[w, half, k, d],
                                            device_id=plane_peer(along_y, d), device_id_type=MESH)

    def plane_open(w):
        for half in range(2):
            for d in (1, 3, 2):
                plane_copy(w, half, True, 0, d).start()
        for half in range(2):
            for d in (1, 3, 2):
                plane_copy(w, half, False, 0, d).start()

    def plane_forward(w):
        for d in (1, 3, 2):
            for half in range(2):
                plane_copy(w, half, True, 0, d).wait_recv()
                for e in (1, 3, 2):
                    plane_copy(w, half, False, RING - d, e).start()

    def plane_close(w):
        for half in range(2):
            for origin in (0, 3, 1, 2):
                for d in (1, 3, 2):
                    plane_copy(w, half, False, origin, d).wait_recv()

    def pair_copy(w, half):
        blk = bias_s.at[core, w, half]
        return pltpu.make_async_remote_copy(src_ref=blk, dst_ref=blk, send_sem=d_send.at[w, half], recv_sem=d_recv.at[w, half],
                                            device_id=dev(col, row + 1 - 2 * core), device_id_type=MESH)

    def project(ck):
        for d in range(1, rows):
            z_copy(d, ck).wait_recv()

        @pl.loop(0, 2)
        def _(jj):
            j = 2 * ck + jj
            a = layer_norm(zr_s[:, j].astype(f32).reshape(n, chan), gamma, beta)
            k_s[j] = jnp.dot(a, wk_ref[...], preferred_element_type=f32).astype(bf16)
            vt_s[j] = lax.dot_general(wt_s[1], a, NT, preferred_element_type=f32).astype(bf16)
            zero = jnp.zeros((hd, TILE), bf16)
            for it in range(nt):
                aq = a.reshape(n // width, nt, sub, chan)[:, it].reshape(TILE, chan)
                a_s[j, it] = aq
                qt = (lax.dot_general(wt_s[0], aq, NT, preferred_element_type=f32) * (1.0 / math.sqrt(hd))).astype(bf16)
                for h in range(heads):
                    qt_s[j, it, h] = jnp.concatenate([qt[h * hd:(h + 1) * hd] if g == h else zero for g in range(heads)], axis=0)

    eye = (lax.broadcasted_iota(jnp.int32, (128, 128), 0) == lax.broadcasted_iota(jnp.int32, (128, 128), 1)).astype(f32).astype(bf16)
    key = lax.broadcasted_iota(jnp.int32, (128, TILE), 0)

    def expand_bias(w):
        @pl.loop(0, 2)
        def _(ch):
            for hh in range(2):
                for half in range(2):
                    val = bias_s[ch, w, half, :, :, hh].reshape(TILE, n // 2)
                    for kt in range(3):
                        lo = half * (n // 2) + kt * 128
                        out = lax.dot_general(eye, val[:, kt * 128:(kt + 1) * 128], NT, preferred_element_type=f32)
                        biasf_s[2 * ch + hh, pl.ds(lo, 128), :] = out + jnp.where(key < kept - lo, 0.0, MASK_FILL)

    chunk = 128

    def fold(x, op):
        return op(x.reshape(x.shape[0] // 8, 8, TILE), axis=0)

    def logits(w, j, h, s_ref, m_ref):
        qt = qt_s[j, w, h]
        top = None
        for lo in range(0, n, chunk):
            s = jnp.dot(k_s[j, lo:lo + chunk, :], qt, preferred_element_type=f32) + biasf_s[h, lo:lo + chunk, :]
            s_ref[lo:lo + chunk, :] = s
            part = fold(s, jnp.max)
            top = part if top is None else jnp.maximum(top, part)
        m_ref[...] = top

    def finish_tile(w, j, h, s_ref, m_ref):
        top = jnp.max(m_ref[...], axis=0, keepdims=True)
        rows_h = pl.ds(pl.multiple_of(h * hd, hd), hd)
        total, o = None, None
        for lo in range(0, n, TILE):
            p = jnp.exp2((s_ref[lo:lo + TILE, :] - top) * LOG2E)
            part = fold(p, jnp.sum)
            total = part if total is None else total + part
            prod = jnp.dot(vt_s[j, rows_h, lo:lo + TILE], p.astype(bf16), preferred_element_type=f32)
            o = prod if o is None else o + prod
        o_s[rows_h, :] = o / jnp.sum(total, axis=0, keepdims=True)

    def out_copy(w, j, d):
        peer = (row + d) % rows
        return pltpu.make_async_remote_copy(src_ref=res_s.at[w, j, peer], dst_ref=out_ref.at[row * cols + j, :, w], send_sem=o_send.at[w, j, d],
                                            recv_sem=o_recv.at[w, j, d], device_id=dev(col, peer), device_id_type=MESH)

    def own_out(w, j):
        return pltpu.make_async_copy(res_s.at[w, j, row], out_ref.at[row * cols + j, :, w], o_send.at[w, j, 0])

    def finish_column(w, j):
        gate = jax.nn.sigmoid(lax.dot_general(wt_s[2], a_s[j, w], NT, preferred_element_type=f32))
        gated = (gate * o_s[...]).astype(bf16)
        update = jnp.dot(wt_s[3], gated, preferred_element_type=f32)
        res = zr_s[:, j, :, w].astype(f32).reshape(TILE, chan) + update.T
        res_s[w, j] = res.astype(bf16).reshape(rows, 2, sub, chan)
        for d in range(1, rows):
            out_copy(w, j, d).start()
        own_out(w, j).start()

    def attend(w, j_lo, j_hi):
        @pl.loop(j_lo, j_hi)
        def _(j):
            @pl.loop(0, heads // 2)
            def _(u):
                h = 2 * u
                logits(w, j, h + 1, s_b, m_b)
                finish_tile(w, j, h, s_a, m_a)
                nxt = jnp.minimum(j * heads + h + 2, cols * heads - 1)
                logits(w, nxt // heads, nxt % heads, s_a, m_a)
                finish_tile(w, j, h + 1, s_b, m_b)
            finish_column(w, j)

    def pair_start(w):
        for half in range(2):
            pair_copy(w, half).start()

    def begin(w):
        for half in range(2):
            pair_copy(w, half).wait_recv()
        expand_bias(w)
        logits(w, 0, 0, s_a, m_a)

    plane_open(0)
    plane_forward(0)
    plane_open(1)
    own_z.wait()
    project(0)
    plane_forward(1)
    plane_open(2)
    project(1)
    plane_close(0)
    pair_start(0)
    project(2)
    begin(0)
    attend(0, 0, cols // 3)
    plane_forward(2)
    attend(0, cols // 3, 2 * cols // 3)
    plane_close(1)
    pair_start(1)
    attend(0, 2 * cols // 3, cols)
    begin(1)
    attend(1, 0, 2 * cols // 3)
    plane_close(2)
    pair_start(2)
    attend(1, 2 * cols // 3, cols)
    begin(2)
    attend(2, 0, cols)

    for d in range(1, rows):
        g_copy(d).wait_send()
        for ck in range(cols // 2):
            z_copy(d, ck).wait_send()
    for w in range(nt):
        for half in range(2):
            pair_copy(w, half).wait_send()
            for d in range(1, RING):
                plane_copy(w, half, True, 0, d).wait_send()
                for origin in range(RING):
                    plane_copy(w, half, False, origin, d).wait_send()

    @pl.loop(0, cols)
    def _(j):
        for w in range(nt):
            for d in range(1, rows):
                out_copy(w, j, d).wait()
            own_out(w, j).wait()


def solution(mesh):
    rows = mesh.shape['row']

    def body(pair_tile, res_mask, ln_gamma, ln_beta, w_q, w_k, w_v, w_b, w_g, w_o):
        block, width, chan = pair_tile.shape
        heads = w_b.shape[1]
        n = block * rows
        cols = width // rows
        bf16, f32 = jnp.bfloat16, jnp.float32
        nt = n // TILE
        sub = width // nt
        zt = jnp.transpose(pair_tile, (1, 0, 2)).reshape(width, 2, nt, sub, chan)
        V = lambda *s, dt=bf16: pltpu.VMEM(s, dt)
        D = lambda *s: pltpu.SemaphoreType.DMA(s)
        out = pl.pallas_call(
            triangle_kernel,
            out_shape=jax.ShapeDtypeStruct((width, 2, nt, sub, chan), bf16),
            in_specs=[pl.BlockSpec(memory_space=pltpu.VMEM)] * 10,
            out_specs=pl.BlockSpec(memory_space=pl.ANY),
            scratch_shapes=[V(rows, cols, 2, nt, sub, chan), V(heads, width, 128, dt=f32), V(2, 2, width, 128),
                            V(rows, 2, width, 128), V(2, nt, 2, RING, RING, 2, sub, n // 2), V(heads, n, TILE, dt=f32),
                            V(4, chan, chan), V(cols, nt, TILE, chan), V(cols, n, chan), V(cols, chan, n),
                            V(cols, nt, heads, chan, TILE), V(n, TILE, dt=f32), V(n, TILE, dt=f32), V(8, TILE, dt=f32), V(8, TILE, dt=f32),
                            V(chan, TILE, dt=f32), V(nt, cols, rows, 2, sub, chan),
                            D(rows), D(rows), D(rows, cols // 2), D(rows, cols // 2), D(nt, 2, RING + 1, RING), D(nt, 2, RING + 1, RING),
                            D(nt, 2), D(nt, 2), D(nt, cols, rows), D(nt, cols, rows), D(1)],
            compiler_params=pltpu.CompilerParams(vmem_limit_bytes=60000 * 1024, collective_id=0, has_side_effects=True),
            name='triangle',
        )(zt, res_mask, ln_gamma.reshape(1, chan), ln_beta.reshape(1, chan), w_q, w_k, w_v, w_b.T, w_g, w_o)
        return jnp.transpose(out.reshape(width, block, chan), (1, 0, 2))

    tile_spec = P(('data', 'row'), 'col', None)
    return jax.shard_map(body, mesh=mesh, in_specs=(tile_spec, P('data'), P(), P(), P(), P(), P(), P(), P(), P()), out_specs=tile_spec, check_vma=False)
```

```python
import math
import jax
import jax.numpy as jnp
from jax import lax
from jax.experimental import pallas as pl
from jax.experimental.pallas import tpu as pltpu
from jax.sharding import PartitionSpec as P

LN_EPS = 1e-5
MASK_FILL = -1e9
LOG2E = math.log2(math.e)
NT = (((1,), (1,)), ((), ()))
MESH = pl.DeviceIdType.MESH
TILE = 256
RING = 4


def layer_norm(z, gamma, beta):
    mean = jnp.mean(z, axis=-1, keepdims=True)
    centred = z - mean
    variance = jnp.mean(centred * centred, axis=-1, keepdims=True)
    return (centred * lax.rsqrt(variance + LN_EPS) * gamma + beta).astype(jnp.bfloat16)


def triangle_kernel(z_ref, mask_ref, gamma_ref, beta_ref, wq_ref, wk_ref, wv_ref, wb_ref, wg_ref, wo_ref, out_ref,
                    zr_s, bst_s, bt_s, gb_s, bias_s, biasf_s, wt_s, wk_s, gate_s, k_s, vt_s, qt_s, s_a, s_b, m_a, m_b, o_s, res_s,
                    g_send, g_recv, z_send, z_recv, p_send, p_near, p_far, d_send, d_recv, o_send, o_recv, loc_sem):
    f32, bf16 = jnp.float32, jnp.bfloat16
    data, col, row = lax.axis_index('data'), lax.axis_index('col'), lax.axis_index('row')
    rows, cols, chan = zr_s.shape[0], zr_s.shape[1], zr_s.shape[-1]
    width = rows * cols
    block = z_ref.shape[1] * z_ref.shape[2] * z_ref.shape[3]
    n = rows * block
    heads = wb_ref.shape[0]
    hd = chan // heads
    nt = n // TILE
    sub = width // nt
    core = row % 2
    zc, yc = col // RING, col % RING

    def dev(c, r):
        return (data, c, r)

    def row_peer(d):
        return dev(col, (row + d) % rows)

    def plane_peer(along_y, d):
        if along_y:
            return dev(zc * RING + (yc + d) % RING, row)
        return dev((zc + d) % RING * RING + yc, row)

    barrier = pltpu.get_barrier_semaphore()
    for d in range(1, rows):
        pl.semaphore_signal(barrier, inc=1, device_id=row_peer(d), device_id_type=MESH)
    for along_y in (True, False):
        for d in range(1, RING):
            pl.semaphore_signal(barrier, inc=1, device_id=plane_peer(along_y, d), device_id_type=MESH)

    gamma, beta = gamma_ref[...], beta_ref[...]
    wbt = wb_ref[...]
    bst_s[...] = jnp.zeros_like(bst_s)
    group = 8

    @pl.loop(0, width // group)
    def _(g):
        a = layer_norm(z_ref[pl.ds(g * group, group)].astype(f32).reshape(group * block, chan), gamma, beta)
        for t in range(group):
            b = lax.dot_general(wbt, a[t * block:(t + 1) * block], NT, preferred_element_type=f32)
            for h in range(heads):
                bst_s[h, pl.ds(g * group + t, 1), :block] = b[h:h + 1]

    for h in range(heads):
        bt_s[h // 2, h % 2] = bst_s[h].astype(bf16)

    pl.semaphore_wait(barrier, rows - 1 + 2 * (RING - 1))

    def wait_bytes(ref, sem):
        pltpu.make_async_copy(ref, ref, sem).wait()

    def g_copy(d):
        peer = (row + d) % rows
        return pltpu.make_async_remote_copy(src_ref=bt_s.at[peer % 2], dst_ref=gb_s.at[d], send_sem=g_send.at[0], recv_sem=g_recv.at[0],
                                            device_id=dev(col, peer), device_id_type=MESH)

    def z_copy(d, ck):
        peer = (row + d) % rows
        return pltpu.make_async_remote_copy(src_ref=z_ref.at[pl.ds(peer * cols + 2 * ck, 2)], dst_ref=zr_s.at[row, pl.ds(2 * ck, 2)],
                                            send_sem=z_send.at[0], recv_sem=z_recv.at[ck], device_id=dev(col, peer), device_id_type=MESH)

    for d in range(1, rows):
        g_copy(d).start()
    own_z = pltpu.make_async_copy(z_ref.at[pl.ds(row * cols, cols)], zr_s.at[row], loc_sem.at[0])
    own_z.start()

    for idx, w in enumerate((wq_ref, wv_ref, wg_ref, wo_ref)):
        wt_s[idx] = w[...].astype(f32).T.astype(bf16)
    src_id = lax.broadcasted_iota(jnp.int32, (chan, 128), 0)
    dst_id = lax.broadcasted_iota(jnp.int32, (chan, 128), 1)
    for h in range(heads):
        pick = ((src_id == h * hd + dst_id % hd) & (dst_id < 3 * hd)).astype(f32).astype(bf16)
        wk_s[:, h * 128:(h + 1) * 128] = jnp.dot(wk_ref[...], pick, preferred_element_type=f32).astype(bf16)
    kept = jnp.sum(mask_ref[...].reshape(1, n), axis=1, keepdims=True)
    gb_s[0] = bt_s[core]

    wait_bytes(gb_s.at[pl.ds(0, rows - 1)], g_recv.at[0])
    for ck in range(cols // 2):
        for d in range(1, rows):
            z_copy(d, ck).start()
    lane = lax.broadcasted_iota(jnp.int32, (width, 128), 1)
    for hh in range(2):
        for half in range(2):
            for t in range(3):
                lo = half * 4 + t
                first = gb_s[(row - lo + rows) % rows, hh].astype(f32)
                second = gb_s[(row - lo - 1 + rows) % rows, hh].astype(f32)
                cut = block - 32 * t
                piece = jnp.where(lane < cut, pltpu.roll(first, (128 - 32 * t) % 128, 1), pltpu.roll(second, cut, 1))
                for it in range(nt):
                    bias_s[core, it, half, zc, yc, hh, :, t * 128:(t + 1) * 128] = piece[it * sub:(it + 1) * sub].astype(bf16)

    def plane_copy(w, half, first, origin, d):
        along_y = (half == 0) == first
        oz, oy = (zc, (yc + origin) % RING) if half == 0 else ((zc + origin) % RING, yc)
        blk = bias_s.at[core, w, half, oz, oy]
        recv = p_near.at[w, half] if first else p_far.at[w, half, d]
        return pltpu.make_async_remote_copy(src_ref=blk, dst_ref=blk, send_sem=p_send.at[0 if first else 1], recv_sem=recv,
                                            device_id=plane_peer(along_y, d), device_id_type=MESH)

    def pair_copy(w, half, d):
        if half == 0:
            blk = bias_s.at[core, w, half, (zc - d + RING) % RING]
        else:
            blk = bias_s.at[core, w, half, :, (yc - d + RING) % RING]
        return pltpu.make_async_remote_copy(src_ref=blk, dst_ref=blk, send_sem=d_send.at[0], recv_sem=d_recv.at[w],
                                            device_id=dev(col, row + 1 - 2 * core), device_id_type=MESH)

    def plane_open(w):
        for first in (True, False):
            for half in range(2):
                for d in (1, 3, 2):
                    plane_copy(w, half, first, 0, d).start()

    def plane_forward(w):
        for half in range(2):
            wait_bytes(bias_s.at[0, w, half, 0, pl.ds(0, RING - 1)], p_near.at[w, half])
            for origin in range(1, RING):
                for e in (1, 3, 2):
                    plane_copy(w, half, False, origin, e).start()
            pair_copy(w, half, 0).start()

    def plane_close(w):
        for e in (1, 3, 2):
            for half in range(2):
                wait_bytes(bias_s.at[0, w, half, 0], p_far.at[w, half, e])
                pair_copy(w, half, e).start()

    def project(ck):
        wait_bytes(zr_s.at[pl.ds(0, rows - 1), pl.ds(0, 2)], z_recv.at[ck])

        @pl.loop(0, 2)
        def _(jj):
            j = 2 * ck + jj
            a = layer_norm(zr_s[:, j].astype(f32).reshape(n, chan), gamma, beta)
            keys = jnp.dot(a, wk_s[...], preferred_element_type=f32).astype(bf16)
            for h in range(heads):
                k_s[j, h] = keys[:, h * 128:(h + 1) * 128]
            vt_s[j] = lax.dot_general(wt_s[1], a, NT, preferred_element_type=f32).astype(bf16)
            zero = jnp.zeros((hd, TILE), bf16)
            for it in range(nt):
                aq = a.reshape(n // width, nt, sub, chan)[:, it].reshape(TILE, chan)
                gate_s[j, it] = jax.nn.sigmoid(lax.dot_general(wt_s[2], aq, NT, preferred_element_type=f32))
                qt = (lax.dot_general(wt_s[0], aq, NT, preferred_element_type=f32) * (1.0 / math.sqrt(hd))).astype(bf16)
                scaled = qt.astype(f32) * LOG2E
                top = scaled.astype(bf16)
                rest = scaled - top.astype(f32)
                mid = rest.astype(bf16)
                low = (rest - mid.astype(f32)).astype(bf16)
                for h in range(heads):
                    own = slice(h * hd, (h + 1) * hd)
                    qt_s[j, it, h] = jnp.concatenate([top[own], mid[own], low[own], zero], axis=0)

    eye = (lax.broadcasted_iota(jnp.int32, (128, 128), 0) == lax.broadcasted_iota(jnp.int32, (128, 128), 1)).astype(f32).astype(bf16)
    key = lax.broadcasted_iota(jnp.int32, (128, TILE), 0)

    def expand_bias(w):
        @pl.loop(0, 2)
        def _(ch):
            for hh in range(2):
                for half in range(2):
                    val = bias_s[ch, w, half, :, :, hh].reshape(TILE, n // 2)
                    for kt in range(3):
                        lo = half * (n // 2) + kt * 128
                        out = lax.dot_general(eye, val[:, kt * 128:(kt + 1) * 128], NT, preferred_element_type=f32)
                        biasf_s[2 * ch + hh, pl.ds(lo, 128), :] = (out + jnp.where(key < kept - lo, 0.0, MASK_FILL)) * LOG2E

    chunk = 128

    def fold(x, op):
        return op(x.reshape(x.shape[0] // 8, 8, TILE), axis=0)

    def logits(w, j, h, s_ref, m_ref):
        qt = qt_s[j, w, h]
        top = None
        for lo in range(0, n, chunk):
            s = jnp.dot(k_s[j, h, lo:lo + chunk, :], qt, preferred_element_type=f32) + biasf_s[h, lo:lo + chunk, :]
            s_ref[lo:lo + chunk, :] = s
            part = fold(s, jnp.max)
            top = part if top is None else jnp.maximum(top, part)
        m_ref[...] = top

    def finish_tile(w, j, h, s_ref, m_ref):
        top = jnp.max(m_ref[...], axis=0, keepdims=True)
        rows_h = pl.ds(pl.multiple_of(h * hd, hd), hd)
        total, o = None, None
        for lo in range(0, n, TILE):
            p = jnp.exp2(s_ref[lo:lo + TILE, :] - top)
            part = fold(p, jnp.sum)
            total = part if total is None else total + part
            prod = jnp.dot(vt_s[j, rows_h, lo:lo + TILE], p.astype(bf16), preferred_element_type=f32)
            o = prod if o is None else o + prod
        o_s[j, rows_h, :] = o / jnp.sum(total, axis=0, keepdims=True)

    def out_copy(w, j, d):
        peer = (row + d) % rows
        return pltpu.make_async_remote_copy(src_ref=res_s.at[w, j, peer], dst_ref=out_ref.at[row * cols + j, :, w], send_sem=o_send.at[0],
                                            recv_sem=o_recv.at[0], device_id=dev(col, peer), device_id_type=MESH)

    def finish_column(w, j):
        gated = (gate_s[j, w] * o_s[j]).astype(bf16)
        update = jnp.dot(wt_s[3], gated, preferred_element_type=f32)
        res = zr_s[:, j, :, w].astype(f32).reshape(TILE, chan) + update.T
        res_s[w, j] = res.astype(bf16).reshape(rows, 2, sub, chan)

    def send_column(w, j):
        for d in range(1, rows):
            out_copy(w, j, d).start()
        pltpu.make_async_copy(res_s.at[w, j, row], out_ref.at[row * cols + j, :, w], loc_sem.at[1]).start()

    def column(w, j, prev):
        if prev is not None:
            finish_column(*prev)
        for h in range(heads):
            here, there = ((s_a, m_a), (s_b, m_b)) if h % 2 == 0 else ((s_b, m_b), (s_a, m_a))
            if h < heads - 1:
                logits(w, j, h + 1, *there)
            else:
                logits(w, jnp.minimum(j + 1, cols - 1), 0, *there)
            finish_tile(w, j, h, *here)
        if prev is not None:
            send_column(*prev)

    def attend(w, j_lo, j_hi):
        @pl.loop(j_lo, j_hi)
        def _(j):
            column(w, j, (w, j - 1))

    def begin(w):
        wait_bytes(bias_s.at[0, w], d_recv.at[w])
        expand_bias(w)
        logits(w, 0, 0, s_a, m_a)

    last = cols - 1
    plane_open(0)
    plane_forward(0)
    plane_open(1)
    own_z.wait()
    project(0)
    plane_close(0)
    begin(0)
    column(0, 0, None)
    plane_forward(1)
    plane_open(2)
    attend(0, 1, 2)
    project(1)
    logits(0, 2, 0, s_a, m_a)
    attend(0, 2, 4)
    plane_close(1)
    plane_forward(2)
    project(2)
    logits(0, 4, 0, s_a, m_a)
    attend(0, 4, cols)
    begin(1)
    column(1, 0, (0, last))
    attend(1, 1, 3)
    plane_close(2)
    attend(1, 3, cols)
    begin(2)
    column(2, 0, (1, last))
    attend(2, 1, cols)
    finish_column(2, last)
    send_column(2, last)

    wait_bytes(gb_s.at[pl.ds(0, rows - 1)], g_send.at[0])
    wait_bytes(zr_s.at[pl.ds(0, rows - 1)], z_send.at[0])
    wait_bytes(bias_s.at[0, :, :, 0, pl.ds(0, RING - 1)], p_send.at[0])
    wait_bytes(bias_s.at[0, :, :, pl.ds(0, RING - 1)], p_send.at[1])
    wait_bytes(bias_s.at[0], d_send.at[0])
    wait_bytes(res_s.at[:, :, pl.ds(0, 1)], loc_sem.at[1])
    wait_bytes(res_s.at[:, :, pl.ds(0, rows - 1)], o_send.at[0])
    wait_bytes(res_s.at[:, :, pl.ds(0, rows - 1)], o_recv.at[0])


def solution(mesh):
    rows = mesh.shape['row']

    def body(pair_tile, res_mask, ln_gamma, ln_beta, w_q, w_k, w_v, w_b, w_g, w_o):
        block, width, chan = pair_tile.shape
        heads = w_b.shape[1]
        n = block * rows
        cols = width // rows
        bf16, f32 = jnp.bfloat16, jnp.float32
        nt = n // TILE
        sub = width // nt
        zt = jnp.transpose(pair_tile, (1, 0, 2)).reshape(width, 2, nt, sub, chan)
        V = lambda *s, dt=bf16: pltpu.VMEM(s, dt)
        D = lambda *s: pltpu.SemaphoreType.DMA(s)
        out = pl.pallas_call(
            triangle_kernel,
            out_shape=jax.ShapeDtypeStruct((width, 2, nt, sub, chan), bf16),
            in_specs=[pl.BlockSpec(memory_space=pltpu.VMEM)] * 10,
            out_specs=pl.BlockSpec(memory_space=pl.ANY),
            scratch_shapes=[V(rows, cols, 2, nt, sub, chan), V(heads, width, 128, dt=f32), V(2, 2, width, 128),
                            V(rows, 2, width, 128), V(2, nt, 2, RING, RING, 2, sub, n // 2), V(heads, n, TILE, dt=f32),
                            V(4, chan, chan), V(chan, heads * 128), V(cols, nt, chan, TILE, dt=f32), V(cols, heads, n, 128), V(cols, chan, n),
                            V(cols, nt, heads, 128, TILE), V(n, TILE, dt=f32), V(n, TILE, dt=f32), V(8, TILE, dt=f32), V(8, TILE, dt=f32),
                            V(cols, chan, TILE, dt=f32), V(nt, cols, rows, 2, sub, chan),
                            D(1), D(1), D(1), D(cols // 2), D(2), D(nt, 2), D(nt, 2, RING), D(1), D(nt), D(1), D(1), D(2)],
            compiler_params=pltpu.CompilerParams(vmem_limit_bytes=60000 * 1024, collective_id=0, has_side_effects=True),
            name='triangle',
        )(zt, res_mask, ln_gamma.reshape(1, chan), ln_beta.reshape(1, chan), w_q, w_k, w_v, w_b.T, w_g, w_o)
        return jnp.transpose(out.reshape(width, block, chan), (1, 0, 2))

    tile_spec = P(('data', 'row'), 'col', None)
    return jax.shard_map(body, mesh=mesh, in_specs=(tile_spec, P('data'), P(), P(), P(), P(), P(), P(), P(), P()), out_specs=tile_spec, check_vma=False)
```

```python
import math
import jax
import jax.numpy as jnp
from jax import lax
from jax.experimental import pallas as pl
from jax.experimental.pallas import tpu as pltpu
from jax.sharding import PartitionSpec as P

LN_EPS = 1e-5
MASK_FILL = -1e9
LOG2E = math.log2(math.e)
NT = (((1,), (1,)), ((), ()))
MESH = pl.DeviceIdType.MESH
TILE = 256
RING = 4


def layer_norm(z, gamma, beta):
    mean = jnp.mean(z, axis=-1, keepdims=True)
    centred = z - mean
    variance = jnp.mean(centred * centred, axis=-1, keepdims=True)
    return (centred * lax.rsqrt(variance + LN_EPS) * gamma + beta).astype(jnp.bfloat16)


def triangle_kernel(z_ref, mask_ref, gamma_ref, beta_ref, wq_ref, wk_ref, wv_ref, wb_ref, wg_ref, wo_ref, out_ref,
                    zf_s, af_s, zt_s, zr_s, bst_s, bt_s, gb_s, bias_s, biasf_s, wt_s, wk_s, gate_s, k_s, vt_s, qt_s, s_a, s_b, m_a, m_b, o_s, res_s,
                    g_send, g_recv, z_send, z_recv, p_send, p_near, p_far, d_send, d_recv, o_send, o_recv, loc_sem):
    f32, bf16 = jnp.float32, jnp.bfloat16
    data, col, row = lax.axis_index('data'), lax.axis_index('col'), lax.axis_index('row')
    rows, cols, chan = zr_s.shape[0], zr_s.shape[1], zr_s.shape[-1]
    width = rows * cols
    block = z_ref.shape[0]
    n = rows * block
    heads = wb_ref.shape[0]
    hd = chan // heads
    nt = n // TILE
    sub = width // nt
    core = row % 2
    zc, yc = col // RING, col % RING

    def dev(c, r):
        return (data, c, r)

    def row_peer(d):
        return dev(col, (row + d) % rows)

    def plane_peer(along_y, d):
        if along_y:
            return dev(zc * RING + (yc + d) % RING, row)
        return dev((zc + d) % RING * RING + yc, row)

    barrier = pltpu.get_barrier_semaphore()
    for d in range(1, rows):
        pl.semaphore_signal(barrier, inc=1, device_id=row_peer(d), device_id_type=MESH)
    for along_y in (True, False):
        for d in range(1, RING):
            pl.semaphore_signal(barrier, inc=1, device_id=plane_peer(along_y, d), device_id_type=MESH)

    gamma, beta = gamma_ref[...], beta_ref[...]
    wbt = wb_ref[...]
    bst_s[...] = jnp.zeros_like(bst_s)

    def make_bias(w):
        half_rows = block // 2

        @pl.loop(0, 2)
        def _(c):
            z = z_ref[pl.ds(c * half_rows, half_rows), w * sub:(w + 1) * sub, :].astype(f32).reshape(half_rows * sub, chan)
            here = pl.ds(pl.multiple_of(c * half_rows * sub, half_rows * sub), half_rows * sub)
            zf_s[w, here, :] = z
            af_s[here, :] = layer_norm(z, gamma, beta).astype(f32)

        for t in range(sub):
            b = lax.dot_general(wbt, af_s[pl.ds(t, block, stride=sub), :].astype(bf16), NT, preferred_element_type=f32)
            for h in range(heads):
                bst_s[h, pl.ds(t, 1), :block] = b[h:h + 1]
        for h in range(heads):
            bt_s[h // 2, w, h % 2] = bst_s[h].astype(bf16)

    def transpose_z(w):
        for t in range(sub):
            col_z = zf_s[w, pl.ds(t, block, stride=sub), :].astype(bf16)
            zt_s[w * sub + t] = col_z.reshape(2, nt, sub, chan)

    def wait_bytes(ref, sem):
        pltpu.make_async_copy(ref, ref, sem).wait()

    def g_copy(w, d):
        peer = (row + d) % rows
        return pltpu.make_async_remote_copy(src_ref=bt_s.at[peer % 2, w], dst_ref=gb_s.at[w, d], send_sem=g_send.at[0], recv_sem=g_recv.at[w],
                                            device_id=dev(col, peer), device_id_type=MESH)

    def g_start(w):
        for d in range(1, rows):
            g_copy(w, d).start()

    def z_start(ck):
        for d in range(1, rows):
            z_copy(d, ck).start()

    def z_copy(d, ck):
        peer = (row + d) % rows
        return pltpu.make_async_remote_copy(src_ref=zt_s.at[pl.ds(peer * cols + 2 * ck, 2)], dst_ref=zr_s.at[row, pl.ds(2 * ck, 2)],
                                            send_sem=z_send.at[0], recv_sem=z_recv.at[ck], device_id=dev(col, peer), device_id_type=MESH)

    make_bias(0)
    pl.semaphore_wait(barrier, rows - 1 + 2 * (RING - 1))
    g_start(0)
    for w in range(1, nt):
        make_bias(w)
        g_start(w)
    for w in range(nt):
        transpose_z(w)
    z_start(0)
    own_z = pltpu.make_async_copy(zt_s.at[pl.ds(row * cols, cols)], zr_s.at[row], loc_sem.at[0])
    own_z.start()

    for idx, w in enumerate((wq_ref, wv_ref, wg_ref, wo_ref)):
        wt_s[idx] = w[...].astype(f32).T.astype(bf16)
    src_id = lax.broadcasted_iota(jnp.int32, (chan, 128), 0)
    dst_id = lax.broadcasted_iota(jnp.int32, (chan, 128), 1)
    for h in range(heads):
        pick = ((src_id == h * hd + dst_id % hd) & (dst_id < 3 * hd)).astype(f32).astype(bf16)
        wk_s[:, h * 128:(h + 1) * 128] = jnp.dot(wk_ref[...], pick, preferred_element_type=f32).astype(bf16)
    kept = jnp.sum(mask_ref[...].reshape(1, n), axis=1, keepdims=True)
    lane = lax.broadcasted_iota(jnp.int32, (sub, 128), 1)

    def assemble(w):
        gb_s[w, 0] = bt_s[core, w]
        wait_bytes(gb_s.at[w, pl.ds(0, rows - 1)], g_recv.at[w])
        for hh in range(2):
            for half in range(2):
                for t in range(3):
                    lo = half * 4 + t
                    first = gb_s[w, (row - lo + rows) % rows, hh].astype(f32)
                    second = gb_s[w, (row - lo - 1 + rows) % rows, hh].astype(f32)
                    cut = block - 32 * t
                    piece = jnp.where(lane < cut, pltpu.roll(first, (128 - 32 * t) % 128, 1), pltpu.roll(second, cut, 1))
                    bias_s[core, w, half, zc, yc, hh, :, t * 128:(t + 1) * 128] = piece.astype(bf16)

    def plane_copy(w, half, first, origin, d):
        along_y = (half == 0) == first
        oz, oy = (zc, (yc + origin) % RING) if half == 0 else ((zc + origin) % RING, yc)
        blk = bias_s.at[core, w, half, oz, oy]
        recv = p_near.at[w, half] if first else p_far.at[w, half, d]
        return pltpu.make_async_remote_copy(src_ref=blk, dst_ref=blk, send_sem=p_send.at[0 if first else 1], recv_sem=recv,
                                            device_id=plane_peer(along_y, d), device_id_type=MESH)

    def pair_copy(w, half, d):
        if half == 0:
            blk = bias_s.at[core, w, half, (zc - d + RING) % RING]
        else:
            blk = bias_s.at[core, w, half, :, (yc - d + RING) % RING]
        return pltpu.make_async_remote_copy(src_ref=blk, dst_ref=blk, send_sem=d_send.at[0], recv_sem=d_recv.at[w],
                                            device_id=dev(col, row + 1 - 2 * core), device_id_type=MESH)

    def plane_open(w):
        for first in (True, False):
            for half in range(2):
                for d in (1, 3, 2):
                    plane_copy(w, half, first, 0, d).start()

    def plane_forward(w):
        for half in range(2):
            wait_bytes(bias_s.at[0, w, half, 0, pl.ds(0, RING - 1)], p_near.at[w, half])
            for origin in range(1, RING):
                for e in (1, 3, 2):
                    plane_copy(w, half, False, origin, e).start()
            pair_copy(w, half, 0).start()

    def plane_close(w):
        for e in (1, 3, 2):
            for half in range(2):
                wait_bytes(bias_s.at[0, w, half, 0], p_far.at[w, half, e])
                pair_copy(w, half, e).start()

    def project(ck):
        wait_bytes(zr_s.at[pl.ds(0, rows - 1), pl.ds(0, 2)], z_recv.at[ck])

        @pl.loop(0, 2)
        def _(jj):
            j = 2 * ck + jj
            a = layer_norm(zr_s[:, j].astype(f32).reshape(n, chan), gamma, beta)
            keys = jnp.dot(a, wk_s[...], preferred_element_type=f32).astype(bf16)
            for h in range(heads):
                k_s[j, h] = keys[:, h * 128:(h + 1) * 128]
            vt_s[j] = lax.dot_general(wt_s[1], a, NT, preferred_element_type=f32).astype(bf16)
            zero = jnp.zeros((hd, TILE), bf16)
            for it in range(nt):
                aq = a.reshape(n // width, nt, sub, chan)[:, it].reshape(TILE, chan)
                gate_s[j, it] = jax.nn.sigmoid(lax.dot_general(wt_s[2], aq, NT, preferred_element_type=f32))
                qt = (lax.dot_general(wt_s[0], aq, NT, preferred_element_type=f32) * (1.0 / math.sqrt(hd))).astype(bf16)
                scaled = qt.astype(f32) * LOG2E
                top = scaled.astype(bf16)
                rest = scaled - top.astype(f32)
                mid = rest.astype(bf16)
                low = (rest - mid.astype(f32)).astype(bf16)
                for h in range(heads):
                    own = slice(h * hd, (h + 1) * hd)
                    qt_s[j, it, h] = jnp.concatenate([top[own], mid[own], low[own], zero], axis=0)

    eye = (lax.broadcasted_iota(jnp.int32, (128, 128), 0) == lax.broadcasted_iota(jnp.int32, (128, 128), 1)).astype(f32).astype(bf16)
    key = lax.broadcasted_iota(jnp.int32, (128, TILE), 0)

    def expand_bias(w):
        @pl.loop(0, 2)
        def _(ch):
            for hh in range(2):
                for half in range(2):
                    val = bias_s[ch, w, half, :, :, hh].reshape(TILE, n // 2)
                    for kt in range(3):
                        lo = half * (n // 2) + kt * 128
                        out = lax.dot_general(eye, val[:, kt * 128:(kt + 1) * 128], NT, preferred_element_type=f32)
                        biasf_s[2 * ch + hh, pl.ds(lo, 128), :] = (out + jnp.where(key < kept - lo, 0.0, MASK_FILL)) * LOG2E

    chunk = 128

    def fold(x, op):
        return op(x.reshape(x.shape[0] // 8, 8, TILE), axis=0)

    def logits(w, j, h, s_ref, m_ref):
        qt = qt_s[j, w, h]
        top = None
        for lo in range(0, n, chunk):
            s = jnp.dot(k_s[j, h, lo:lo + chunk, :], qt, preferred_element_type=f32) + biasf_s[h, lo:lo + chunk, :]
            s_ref[lo:lo + chunk, :] = s
            part = fold(s, jnp.max)
            top = part if top is None else jnp.maximum(top, part)
        m_ref[...] = top

    def finish_tile(w, j, h, s_ref, m_ref):
        top = jnp.max(m_ref[...], axis=0, keepdims=True)
        rows_h = pl.ds(pl.multiple_of(h * hd, hd), hd)
        total, o = None, None
        for lo in range(0, n, chunk):
            p = jnp.exp2(s_ref[lo:lo + chunk, :] - top)
            part = fold(p, jnp.sum)
            total = part if total is None else total + part
            prod = jnp.dot(vt_s[j, rows_h, lo:lo + chunk], p.astype(bf16), preferred_element_type=f32)
            o = prod if o is None else o + prod
        o_s[j, rows_h, :] = o / jnp.sum(total, axis=0, keepdims=True)

    def out_copy(w, j, d):
        peer = (row + d) % rows
        return pltpu.make_async_remote_copy(src_ref=res_s.at[w, j, peer], dst_ref=out_ref.at[row * cols + j, :, w], send_sem=o_send.at[0],
                                            recv_sem=o_recv.at[0], device_id=dev(col, peer), device_id_type=MESH)

    def finish_column(w, j):
        gated = (gate_s[j, w] * o_s[j]).astype(bf16)
        update = jnp.dot(wt_s[3], gated, preferred_element_type=f32)
        res = zr_s[:, j, :, w].astype(f32).reshape(TILE, chan) + update.T
        res_s[w, j] = res.astype(bf16).reshape(rows, 2, sub, chan)

    def send_column(w, j):
        for d in range(1, rows):
            out_copy(w, j, d).start()
        pltpu.make_async_copy(res_s.at[w, j, row], out_ref.at[row * cols + j, :, w], loc_sem.at[1]).start()

    def column(w, j, prev):
        if prev is not None:
            finish_column(*prev)
        for h in range(heads):
            here, there = ((s_a, m_a), (s_b, m_b)) if h % 2 == 0 else ((s_b, m_b), (s_a, m_a))
            if h < heads - 1:
                logits(w, j, h + 1, *there)
            else:
                logits(w, jnp.minimum(j + 1, cols - 1), 0, *there)
            finish_tile(w, j, h, *here)
        if prev is not None:
            send_column(*prev)

    def attend(w, j_lo, j_hi):
        @pl.loop(j_lo, j_hi)
        def _(j):
            column(w, j, (w, j - 1))

    def begin(w):
        wait_bytes(bias_s.at[0, w], d_recv.at[w])
        expand_bias(w)
        logits(w, 0, 0, s_a, m_a)

    last = cols - 1
    assemble(0)
    plane_open(0)
    z_start(1)
    z_start(2)
    assemble(1)
    assemble(2)
    plane_forward(0)
    plane_open(1)
    own_z.wait()
    project(0)
    plane_close(0)
    project(1)
    begin(0)
    column(0, 0, None)
    plane_forward(1)
    plane_open(2)
    attend(0, 1, 4)
    plane_close(1)
    plane_forward(2)
    project(2)
    logits(0, 4, 0, s_a, m_a)
    attend(0, 4, cols)
    begin(1)
    column(1, 0, (0, last))
    attend(1, 1, 3)
    plane_close(2)
    attend(1, 3, cols)
    begin(2)
    column(2, 0, (1, last))
    attend(2, 1, cols)
    finish_column(2, last)
    send_column(2, last)

    wait_bytes(gb_s.at[:, pl.ds(0, rows - 1)], g_send.at[0])
    wait_bytes(zr_s.at[pl.ds(0, rows - 1)], z_send.at[0])
    wait_bytes(bias_s.at[0, :, :, 0, pl.ds(0, RING - 1)], p_send.at[0])
    wait_bytes(bias_s.at[0, :, :, pl.ds(0, RING - 1)], p_send.at[1])
    wait_bytes(bias_s.at[0], d_send.at[0])
    wait_bytes(res_s.at[:, :, pl.ds(0, 1)], loc_sem.at[1])
    wait_bytes(res_s.at[:, :, pl.ds(0, rows - 1)], o_send.at[0])
    wait_bytes(res_s.at[:, :, pl.ds(0, rows - 1)], o_recv.at[0])


def solution(mesh):
    rows = mesh.shape['row']

    def body(pair_tile, res_mask, ln_gamma, ln_beta, w_q, w_k, w_v, w_b, w_g, w_o):
        block, width, chan = pair_tile.shape
        heads = w_b.shape[1]
        n = block * rows
        cols = width // rows
        bf16, f32 = jnp.bfloat16, jnp.float32
        nt = n // TILE
        sub = width // nt
        V = lambda *s, dt=bf16: pltpu.VMEM(s, dt)
        D = lambda *s: pltpu.SemaphoreType.DMA(s)
        out = pl.pallas_call(
            triangle_kernel,
            out_shape=jax.ShapeDtypeStruct((width, 2, nt, sub, chan), bf16),
            in_specs=[pl.BlockSpec(memory_space=pltpu.VMEM)] * 10,
            out_specs=pl.BlockSpec(memory_space=pl.ANY),
            scratch_shapes=[V(nt, block * sub, chan, dt=f32), V(block * sub, chan, dt=f32), V(width, 2, nt, sub, chan),
                            V(rows, cols, 2, nt, sub, chan), V(heads, sub, 128, dt=f32), V(2, nt, 2, sub, 128),
                            V(nt, rows, 2, sub, 128), V(2, nt, 2, RING, RING, 2, sub, n // 2), V(heads, n, TILE, dt=f32),
                            V(4, chan, chan), V(chan, heads * 128), V(cols, nt, chan, TILE, dt=f32), V(cols, heads, n, 128), V(cols, chan, n),
                            V(cols, nt, heads, 128, TILE), V(n, TILE, dt=f32), V(n, TILE, dt=f32), V(8, TILE, dt=f32), V(8, TILE, dt=f32),
                            V(cols, chan, TILE, dt=f32), V(nt, cols, rows, 2, sub, chan),
                            D(1), D(nt), D(1), D(cols // 2), D(2), D(nt, 2), D(nt, 2, RING), D(1), D(nt), D(1), D(1), D(2)],
            compiler_params=pltpu.CompilerParams(vmem_limit_bytes=60000 * 1024, collective_id=0,
                                                 has_side_effects=True),
            name='triangle',
        )(pair_tile, res_mask, ln_gamma.reshape(1, chan), ln_beta.reshape(1, chan), w_q, w_k, w_v, w_b.T, w_g, w_o)
        return jnp.transpose(out.reshape(width, block, chan), (1, 0, 2))

    tile_spec = P(('data', 'row'), 'col', None)
    return jax.shard_map(body, mesh=mesh, in_specs=(tile_spec, P('data'), P(), P(), P(), P(), P(), P(), P(), P()), out_specs=tile_spec, check_vma=False)
```

```python
import math
import jax
import jax.numpy as jnp
from jax import lax
from jax.experimental import pallas as pl
from jax.experimental.pallas import tpu as pltpu
from jax.sharding import PartitionSpec as P

LN_EPS = 1e-5
MASK_FILL = -1e9
LOG2E = math.log2(math.e)
NT = (((1,), (1,)), ((), ()))
MESH = pl.DeviceIdType.MESH
TILE = 256
RING = 4


def layer_norm(z, gamma, beta):
    mean = jnp.mean(z, axis=-1, keepdims=True)
    centred = z - mean
    variance = jnp.mean(centred * centred, axis=-1, keepdims=True)
    return (centred * lax.rsqrt(variance + LN_EPS) * gamma + beta).astype(jnp.bfloat16)


def triangle_kernel(z_hbm, mask_hbm, gamma_hbm, beta_hbm, wq_hbm, wk_hbm, wv_hbm, wb_hbm, wg_hbm, wo_hbm, out_ref,
                    z_ref, mask_ref, gamma_ref, beta_ref, wq_ref, wk_ref, wv_ref, wb_ref, wg_ref, wo_ref,
                    zf_s, af_s, zt_s, zr_s, bst_s, bt_s, gb_s, bias_s, biasf_s, wt_s, wk_s, gate_s, k_s, vt_s, qt_s, s_a, s_b, m_a, m_b, o_s, res_s,
                    g_send, g_recv, z_send, z_recv, p_send, p_near, p_far, d_send, d_recv, o_send, o_recv, loc_sem, z_sem, in_sem):
    f32, bf16 = jnp.float32, jnp.bfloat16
    data, col, row = lax.axis_index('data'), lax.axis_index('col'), lax.axis_index('row')
    rows, cols, chan = zr_s.shape[0], zr_s.shape[1], zr_s.shape[-1]
    width = rows * cols
    block = z_ref.shape[0]
    n = rows * block
    heads = wb_ref.shape[0]
    hd = chan // heads
    nt = n // TILE
    sub = width // nt
    core = row % 2
    zc, yc = col // RING, col % RING

    def dev(c, r):
        return (data, c, r)

    def row_peer(d):
        return dev(col, (row + d) % rows)

    def plane_peer(along_y, d):
        if along_y:
            return dev(zc * RING + (yc + d) % RING, row)
        return dev((zc + d) % RING * RING + yc, row)

    barrier = pltpu.get_barrier_semaphore()
    for d in range(1, rows):
        pl.semaphore_signal(barrier, inc=1, device_id=row_peer(d), device_id_type=MESH)
    for along_y in (True, False):
        for d in range(1, RING):
            pl.semaphore_signal(barrier, inc=1, device_id=plane_peer(along_y, d), device_id_type=MESH)

    def load_z(w):
        piece = (slice(None), pl.ds(w * sub, sub))
        return pltpu.make_async_copy(z_hbm.at[piece], z_ref.at[piece], z_sem.at[w])

    small = [pltpu.make_async_copy(src, dst, in_sem.at[idx]) for idx, (src, dst) in enumerate((
        (gamma_hbm, gamma_ref), (beta_hbm, beta_ref), (wb_hbm, wb_ref), (mask_hbm, mask_ref), (wq_hbm, wq_ref), (wk_hbm, wk_ref),
        (wv_hbm, wv_ref), (wg_hbm, wg_ref), (wo_hbm, wo_ref)))]
    load_z(0).start()
    for copy in small:
        copy.start()
    for w in range(1, nt):
        load_z(w).start()
    for copy in small[:3]:
        copy.wait()
    gamma, beta = gamma_ref[...], beta_ref[...]
    wbt = wb_ref[...]
    bst_s[...] = jnp.zeros_like(bst_s)

    def make_bias(w):
        half_rows = block // 2
        load_z(w).wait()

        @pl.loop(0, 2)
        def _(c):
            z = z_ref[pl.ds(c * half_rows, half_rows), w * sub:(w + 1) * sub, :].astype(f32).reshape(half_rows * sub, chan)
            here = pl.ds(pl.multiple_of(c * half_rows * sub, half_rows * sub), half_rows * sub)
            zf_s[w, here, :] = z
            af_s[here, :] = layer_norm(z, gamma, beta).astype(f32)

        for t in range(sub):
            b = lax.dot_general(wbt, af_s[pl.ds(t, block, stride=sub), :].astype(bf16), NT, preferred_element_type=f32)
            for h in range(heads):
                bst_s[h, pl.ds(t, 1), :block] = b[h:h + 1]
        for h in range(heads):
            bt_s[h // 2, w, h % 2] = bst_s[h].astype(bf16)

    def transpose_z(w):
        for t in range(sub):
            col_z = zf_s[w, pl.ds(t, block, stride=sub), :].astype(bf16)
            zt_s[w * sub + t] = col_z.reshape(2, nt, sub, chan)

    def wait_bytes(ref, sem):
        pltpu.make_async_copy(ref, ref, sem).wait()

    def g_copy(w, d):
        peer = (row + d) % rows
        return pltpu.make_async_remote_copy(src_ref=bt_s.at[peer % 2, w], dst_ref=gb_s.at[w, d], send_sem=g_send.at[0], recv_sem=g_recv.at[w],
                                            device_id=dev(col, peer), device_id_type=MESH)

    def g_start(w):
        for d in range(1, rows):
            g_copy(w, d).start()

    def z_start(ck):
        for d in range(1, rows):
            z_copy(d, ck).start()

    def z_copy(d, ck):
        peer = (row + d) % rows
        return pltpu.make_async_remote_copy(src_ref=zt_s.at[pl.ds(peer * cols + 2 * ck, 2)], dst_ref=zr_s.at[row, pl.ds(2 * ck, 2)],
                                            send_sem=z_send.at[0], recv_sem=z_recv.at[ck], device_id=dev(col, peer), device_id_type=MESH)

    make_bias(0)
    pl.semaphore_wait(barrier, rows - 1 + 2 * (RING - 1))
    g_start(0)
    for w in range(1, nt):
        make_bias(w)
    for w in range(nt):
        transpose_z(w)
    own_z = pltpu.make_async_copy(zt_s.at[pl.ds(row * cols, cols)], zr_s.at[row], loc_sem.at[0])
    own_z.start()
    for copy in small[3:]:
        copy.wait()

    for idx, w in enumerate((wq_ref, wv_ref, wg_ref, wo_ref)):
        wt_s[idx] = w[...].astype(f32).T.astype(bf16)
    src_id = lax.broadcasted_iota(jnp.int32, (chan, 128), 0)
    dst_id = lax.broadcasted_iota(jnp.int32, (chan, 128), 1)
    for h in range(heads):
        pick = ((src_id == h * hd + dst_id % hd) & (dst_id < 3 * hd)).astype(f32).astype(bf16)
        wk_s[:, h * 128:(h + 1) * 128] = jnp.dot(wk_ref[...], pick, preferred_element_type=f32).astype(bf16)
    kept = jnp.sum(mask_ref[...].reshape(1, n), axis=1, keepdims=True)
    lane = lax.broadcasted_iota(jnp.int32, (sub, 128), 1)

    def assemble(w):
        gb_s[w, 0] = bt_s[core, w]
        wait_bytes(gb_s.at[w, pl.ds(0, rows - 1)], g_recv.at[w])
        for hh in range(2):
            for half in range(2):
                for t in range(3):
                    lo = half * 4 + t
                    first = gb_s[w, (row - lo + rows) % rows, hh].astype(f32)
                    second = gb_s[w, (row - lo - 1 + rows) % rows, hh].astype(f32)
                    cut = block - 32 * t
                    piece = jnp.where(lane < cut, pltpu.roll(first, (128 - 32 * t) % 128, 1), pltpu.roll(second, cut, 1))
                    bias_s[core, w, half, zc, yc, hh, :, t * 128:(t + 1) * 128] = piece.astype(bf16)

    def plane_copy(w, half, first, origin, d):
        along_y = (half == 0) == first
        oz, oy = (zc, (yc + origin) % RING) if half == 0 else ((zc + origin) % RING, yc)
        blk = bias_s.at[core, w, half, oz, oy]
        recv = p_near.at[w, half] if first else p_far.at[w, half, d]
        return pltpu.make_async_remote_copy(src_ref=blk, dst_ref=blk, send_sem=p_send.at[0 if first else 1], recv_sem=recv,
                                            device_id=plane_peer(along_y, d), device_id_type=MESH)

    def pair_copy(w, half, d):
        if half == 0:
            blk = bias_s.at[core, w, half, (zc - d + RING) % RING]
        else:
            blk = bias_s.at[core, w, half, :, (yc - d + RING) % RING]
        return pltpu.make_async_remote_copy(src_ref=blk, dst_ref=blk, send_sem=d_send.at[0], recv_sem=d_recv.at[w],
                                            device_id=dev(col, row + 1 - 2 * core), device_id_type=MESH)

    def plane_open(w):
        for first in (True, False):
            for half in range(2):
                for d in (1, 3, 2):
                    plane_copy(w, half, first, 0, d).start()

    def plane_forward(w):
        for half in range(2):
            wait_bytes(bias_s.at[0, w, half, 0, pl.ds(0, RING - 1)], p_near.at[w, half])
            for origin in range(1, RING):
                for e in (1, 3, 2):
                    plane_copy(w, half, False, origin, e).start()
            pair_copy(w, half, 0).start()

    def plane_close(w):
        for e in (1, 3, 2):
            for half in range(2):
                wait_bytes(bias_s.at[0, w, half, 0], p_far.at[w, half, e])
                pair_copy(w, half, e).start()

    def project(ck):
        wait_bytes(zr_s.at[pl.ds(0, rows - 1), pl.ds(0, 2)], z_recv.at[ck])

        @pl.loop(0, 2)
        def _(jj):
            j = 2 * ck + jj
            a = layer_norm(zr_s[:, j].astype(f32).reshape(n, chan), gamma, beta)
            keys = jnp.dot(a, wk_s[...], preferred_element_type=f32).astype(bf16)
            for h in range(heads):
                k_s[j, h] = keys[:, h * 128:(h + 1) * 128]
            vt_s[j] = lax.dot_general(wt_s[1], a, NT, preferred_element_type=f32).astype(bf16)
            zero = jnp.zeros((hd, TILE), bf16)
            for it in range(nt):
                aq = a.reshape(n // width, nt, sub, chan)[:, it].reshape(TILE, chan)
                gate_s[j, it] = jax.nn.sigmoid(lax.dot_general(wt_s[2], aq, NT, preferred_element_type=f32))
                qt = (lax.dot_general(wt_s[0], aq, NT, preferred_element_type=f32) * (1.0 / math.sqrt(hd))).astype(bf16)
                scaled = qt.astype(f32) * LOG2E
                top = scaled.astype(bf16)
                rest = scaled - top.astype(f32)
                mid = rest.astype(bf16)
                low = (rest - mid.astype(f32)).astype(bf16)
                for h in range(heads):
                    own = slice(h * hd, (h + 1) * hd)
                    qt_s[j, it, h] = jnp.concatenate([top[own], mid[own], low[own], zero], axis=0)

    eye = (lax.broadcasted_iota(jnp.int32, (128, 128), 0) == lax.broadcasted_iota(jnp.int32, (128, 128), 1)).astype(f32).astype(bf16)
    key = lax.broadcasted_iota(jnp.int32, (128, TILE), 0)

    def expand_bias(w):
        @pl.loop(0, 2)
        def _(ch):
            for hh in range(2):
                for half in range(2):
                    val = bias_s[ch, w, half, :, :, hh].reshape(TILE, n // 2)
                    for kt in range(3):
                        lo = half * (n // 2) + kt * 128
                        out = lax.dot_general(eye, val[:, kt * 128:(kt + 1) * 128], NT, preferred_element_type=f32)
                        biasf_s[2 * ch + hh, pl.ds(lo, 128), :] = (out + jnp.where(key < kept - lo, 0.0, MASK_FILL)) * LOG2E

    chunk = 128

    def fold(x, op):
        return op(x.reshape(x.shape[0] // 8, 8, TILE), axis=0)

    def logits(w, j, h, s_ref, m_ref):
        qt = qt_s[j, w, h]
        top = None
        for lo in range(0, n, chunk):
            s = jnp.dot(k_s[j, h, lo:lo + chunk, :], qt, preferred_element_type=f32) + biasf_s[h, lo:lo + chunk, :]
            s_ref[lo:lo + chunk, :] = s
            part = fold(s, jnp.max)
            top = part if top is None else jnp.maximum(top, part)
        m_ref[...] = top

    def finish_tile(w, j, h, s_ref, m_ref):
        top = jnp.max(m_ref[...], axis=0, keepdims=True)
        rows_h = pl.ds(pl.multiple_of(h * hd, hd), hd)
        total, o = None, None
        for lo in range(0, n, chunk):
            p = jnp.exp2(s_ref[lo:lo + chunk, :] - top)
            part = fold(p, jnp.sum)
            total = part if total is None else total + part
            prod = jnp.dot(vt_s[j, rows_h, lo:lo + chunk], p.astype(bf16), preferred_element_type=f32)
            o = prod if o is None else o + prod
        o_s[j, rows_h, :] = o / jnp.sum(total, axis=0, keepdims=True)

    def out_copy(w, j, d):
        peer = (row + d) % rows
        return pltpu.make_async_remote_copy(src_ref=res_s.at[w, j, peer], dst_ref=out_ref.at[row * cols + j, :, w], send_sem=o_send.at[0],
                                            recv_sem=o_recv.at[0], device_id=dev(col, peer), device_id_type=MESH)

    def finish_column(w, j):
        gated = (gate_s[j, w] * o_s[j]).astype(bf16)
        update = jnp.dot(wt_s[3], gated, preferred_element_type=f32)
        res = zr_s[:, j, :, w].astype(f32).reshape(TILE, chan) + update.T
        res_s[w, j] = res.astype(bf16).reshape(rows, 2, sub, chan)

    def send_column(w, j):
        for d in range(1, rows):
            out_copy(w, j, d).start()
        pltpu.make_async_copy(res_s.at[w, j, row], out_ref.at[row * cols + j, :, w], loc_sem.at[1]).start()

    def column(w, j, prev):
        if prev is not None:
            finish_column(*prev)
        for h in range(heads):
            here, there = ((s_a, m_a), (s_b, m_b)) if h % 2 == 0 else ((s_b, m_b), (s_a, m_a))
            if h < heads - 1:
                logits(w, j, h + 1, *there)
            else:
                logits(w, jnp.minimum(j + 1, cols - 1), 0, *there)
            finish_tile(w, j, h, *here)
        if prev is not None:
            send_column(*prev)

    def attend(w, j_lo, j_hi):
        @pl.loop(j_lo, j_hi)
        def _(j):
            column(w, j, (w, j - 1))

    def begin(w):
        wait_bytes(bias_s.at[0, w], d_recv.at[w])
        expand_bias(w)
        logits(w, 0, 0, s_a, m_a)

    last = cols - 1
    assemble(0)
    plane_open(0)
    for w in range(1, nt):
        g_start(w)
    for ck in range(cols // 2):
        z_start(ck)
    plane_forward(0)
    assemble(1)
    plane_open(1)
    own_z.wait()
    project(0)
    assemble(2)
    plane_close(0)
    plane_forward(1)
    plane_open(2)
    project(1)
    begin(0)
    column(0, 0, None)
    attend(0, 1, 4)
    plane_close(1)
    plane_forward(2)
    project(2)
    logits(0, 4, 0, s_a, m_a)
    attend(0, 4, cols)
    begin(1)
    column(1, 0, (0, last))
    attend(1, 1, 3)
    plane_close(2)
    attend(1, 3, cols)
    begin(2)
    column(2, 0, (1, last))
    attend(2, 1, cols)
    finish_column(2, last)
    send_column(2, last)

    wait_bytes(gb_s.at[:, pl.ds(0, rows - 1)], g_send.at[0])
    wait_bytes(zr_s.at[pl.ds(0, rows - 1)], z_send.at[0])
    wait_bytes(bias_s.at[0, :, :, 0, pl.ds(0, RING - 1)], p_send.at[0])
    wait_bytes(bias_s.at[0, :, :, pl.ds(0, RING - 1)], p_send.at[1])
    wait_bytes(bias_s.at[0], d_send.at[0])
    wait_bytes(res_s.at[:, :, pl.ds(0, 1)], loc_sem.at[1])
    wait_bytes(res_s.at[:, :, pl.ds(0, rows - 1)], o_send.at[0])
    wait_bytes(res_s.at[:, :, pl.ds(0, rows - 1)], o_recv.at[0])


def solution(mesh):
    rows = mesh.shape['row']

    def body(pair_tile, res_mask, ln_gamma, ln_beta, w_q, w_k, w_v, w_b, w_g, w_o):
        block, width, chan = pair_tile.shape
        heads = w_b.shape[1]
        n = block * rows
        cols = width // rows
        bf16, f32 = jnp.bfloat16, jnp.float32
        nt = n // TILE
        sub = width // nt
        V = lambda *s, dt=bf16: pltpu.VMEM(s, dt)
        D = lambda *s: pltpu.SemaphoreType.DMA(s)
        out = pl.pallas_call(
            triangle_kernel,
            out_shape=jax.ShapeDtypeStruct((width, 2, nt, sub, chan), bf16),
            in_specs=[pl.BlockSpec(memory_space=pl.ANY)] * 10,
            out_specs=pl.BlockSpec(memory_space=pl.ANY),
            scratch_shapes=[V(block, width, chan), V(n, dt=jnp.int32), V(1, chan, dt=f32), V(1, chan, dt=f32), V(chan, chan), V(chan, chan),
                            V(chan, chan), V(heads, chan), V(chan, chan), V(chan, chan),
                            V(nt, block * sub, chan, dt=f32), V(block * sub, chan, dt=f32), V(width, 2, nt, sub, chan),
                            V(rows, cols, 2, nt, sub, chan), V(heads, sub, 128, dt=f32), V(2, nt, 2, sub, 128),
                            V(nt, rows, 2, sub, 128), V(2, nt, 2, RING, RING, 2, sub, n // 2), V(heads, n, TILE, dt=f32),
                            V(4, chan, chan), V(chan, heads * 128), V(cols, nt, chan, TILE, dt=f32), V(cols, heads, n, 128), V(cols, chan, n),
                            V(cols, nt, heads, 128, TILE), V(n, TILE, dt=f32), V(n, TILE, dt=f32), V(8, TILE, dt=f32), V(8, TILE, dt=f32),
                            V(cols, chan, TILE, dt=f32), V(nt, cols, rows, 2, sub, chan),
                            D(1), D(nt), D(1), D(cols // 2), D(2), D(nt, 2), D(nt, 2, RING), D(1), D(nt), D(1), D(1), D(2), D(nt), D(9)],
            compiler_params=pltpu.CompilerParams(vmem_limit_bytes=60000 * 1024, collective_id=0,
                                                 has_side_effects=True),
            name='triangle',
        )(pair_tile, res_mask, ln_gamma.reshape(1, chan), ln_beta.reshape(1, chan), w_q, w_k, w_v, w_b.T, w_g, w_o)
        return jnp.transpose(out.reshape(width, block, chan), (1, 0, 2))

    tile_spec = P(('data', 'row'), 'col', None)
    return jax.shard_map(body, mesh=mesh, in_specs=(tile_spec, P('data'), P(), P(), P(), P(), P(), P(), P(), P()), out_specs=tile_spec, check_vma=False)
```

```python
import math
import jax
import jax.numpy as jnp
from jax import lax
from jax.experimental import pallas as pl
from jax.experimental.pallas import tpu as pltpu
from jax.sharding import PartitionSpec as P

LN_EPS = 1e-5
MASK_FILL = -1e9
LOG2E = math.log2(math.e)
NT = (((1,), (1,)), ((), ()))
MESH = pl.DeviceIdType.MESH
TILE = 256
RING = 4


def layer_norm(z, gamma, beta):
    mean = jnp.mean(z, axis=-1, keepdims=True)
    centred = z - mean
    variance = jnp.mean(centred * centred, axis=-1, keepdims=True)
    return (centred * lax.rsqrt(variance + LN_EPS) * gamma + beta).astype(jnp.bfloat16)


def triangle_kernel(z_hbm, mask_hbm, gamma_hbm, beta_hbm, wq_hbm, wk_hbm, wv_hbm, wb_hbm, wg_hbm, wo_hbm, out_ref,
                    z_ref, mask_ref, gamma_ref, beta_ref, wq_ref, wk_ref, wv_ref, wb_ref, wg_ref, wo_ref,
                    zf_s, af_s, zt_s, zr_s, bst_s, bt_s, ga_s, gb_s, bias_s, biasf_s, wt_s, wk_s, gate_s, k_s, vt_s, qt_s, s_a, s_b, m_a, m_b, o_s, res_s,
                    a_send, a_recv, g_send, g_recv, z_send, z_recv, p_send, p_near, p_far, d_send, d_recv, o_send, o_recv, loc_sem, z_sem, in_sem):
    f32, bf16 = jnp.float32, jnp.bfloat16
    data, col, row = lax.axis_index('data'), lax.axis_index('col'), lax.axis_index('row')
    rows, cols, chan = zr_s.shape[0], zr_s.shape[1], zr_s.shape[-1]
    width = rows * cols
    block = z_ref.shape[0]
    n = rows * block
    heads = wb_ref.shape[0]
    hd = chan // heads
    nt = n // TILE
    sub = width // nt
    core = row % 2
    zc, yc = col // RING, col % RING

    def dev(c, r):
        return (data, c, r)

    def row_peer(d):
        return dev(col, (row + d) % rows)

    def plane_peer(along_y, d):
        if along_y:
            return dev(zc * RING + (yc + d) % RING, row)
        return dev((zc + d) % RING * RING + yc, row)

    def plane_device(row_off, along_y, d):
        r = (row + row_off) % rows
        if along_y:
            return dev(zc * RING + (yc + d) % RING, r)
        return dev((zc + d) % RING * RING + yc, r)

    peers = [plane_device(ro, along_y, d) for along_y in (True, False) for d in range(0 if along_y else 1, RING) for ro in range(rows) if d or ro]
    barrier = pltpu.get_barrier_semaphore()
    for peer in peers:
        pl.semaphore_signal(barrier, inc=1, device_id=peer, device_id_type=MESH)

    def load_z(w):
        piece = (slice(None), pl.ds(w * sub, sub))
        return pltpu.make_async_copy(z_hbm.at[piece], z_ref.at[piece], z_sem.at[w])

    small = [pltpu.make_async_copy(src, dst, in_sem.at[idx]) for idx, (src, dst) in enumerate((
        (gamma_hbm, gamma_ref), (beta_hbm, beta_ref), (wb_hbm, wb_ref), (mask_hbm, mask_ref), (wq_hbm, wq_ref), (wk_hbm, wk_ref),
        (wv_hbm, wv_ref), (wg_hbm, wg_ref), (wo_hbm, wo_ref)))]
    load_z(0).start()
    for copy in small:
        copy.start()
    for w in range(1, nt):
        load_z(w).start()
    for copy in small[:3]:
        copy.wait()
    gamma, beta = gamma_ref[...], beta_ref[...]
    wbt = wb_ref[...]
    bst_s[...] = jnp.zeros_like(bst_s)

    def make_bias(w):
        half_rows = block // 2
        if w == 0:
            load_z(w).wait()

        @pl.loop(0, 2)
        def _(c):
            z = z_ref[pl.ds(c * half_rows, half_rows), w * sub:(w + 1) * sub, :].astype(f32).reshape(half_rows * sub, chan)
            here = pl.ds(pl.multiple_of(c * half_rows * sub, half_rows * sub), half_rows * sub)
            if w == 0:
                zf_s[0, here, :] = z
            af_s[here, :] = layer_norm(z, gamma, beta).astype(f32)

        for t in range(sub):
            b = lax.dot_general(wbt, af_s[pl.ds(t, block, stride=sub), :].astype(bf16), NT, preferred_element_type=f32)
            for h in range(heads):
                bst_s[h, pl.ds(t, 1), :block] = b[h:h + 1]
        for h in range(heads):
            bt_s[h // 2, w, h % 2] = bst_s[h].astype(bf16)

    def transpose_z(w):
        if w > 0:
            load_z(w).wait()
            zf_s[w] = z_ref[:, w * sub:(w + 1) * sub, :].astype(f32).reshape(block * sub, chan)
        for t in range(sub):
            col_z = zf_s[w, pl.ds(t, block, stride=sub), :].astype(bf16)
            zt_s[w * sub + t] = col_z.reshape(2, nt, sub, chan)

    def wait_bytes(ref, sem):
        pltpu.make_async_copy(ref, ref, sem).wait()

    my_half = row // RING

    def a_copy(row_off, d):
        peer_row = (row + row_off) % rows
        peer_col = jnp.where(my_half == 0, zc * RING + (yc + d) % RING, (zc + d) % RING * RING + yc)
        slot = my_half * 16 + jnp.where(my_half == 0, yc, zc) * RING + row % RING
        return pltpu.make_async_remote_copy(src_ref=bt_s.at[peer_row % 2, 0], dst_ref=ga_s.at[slot], send_sem=a_send.at[0], recv_sem=a_recv.at[0],
                                            device_id=dev(peer_col, peer_row), device_id_type=MESH)

    def a_start():
        for d in (2, 1, 3, 0):
            for row_off in range(rows):
                if d or row_off:
                    a_copy(row_off, d).start()
        ga_s[my_half * 16 + jnp.where(my_half == 0, yc, zc) * RING + row % RING] = bt_s[core, 0]

    def g_copy(w, d):
        peer = (row + d) % rows
        return pltpu.make_async_remote_copy(src_ref=bt_s.at[peer % 2, w], dst_ref=gb_s.at[w - 1, d], send_sem=g_send.at[0], recv_sem=g_recv.at[w - 1],
                                            device_id=dev(col, peer), device_id_type=MESH)

    def g_start(w):
        for d in range(1, rows):
            g_copy(w, d).start()

    def z_start(ck):
        for d in range(1, rows):
            z_copy(d, ck).start()

    def z_copy(d, ck):
        peer = (row + d) % rows
        return pltpu.make_async_remote_copy(src_ref=zt_s.at[pl.ds(peer * cols + 2 * ck, 2)], dst_ref=zr_s.at[row, pl.ds(2 * ck, 2)],
                                            send_sem=z_send.at[0], recv_sem=z_recv.at[ck], device_id=dev(col, peer), device_id_type=MESH)

    make_bias(0)
    pl.semaphore_wait(barrier, len(peers))
    a_start()
    for w in range(nt):
        transpose_z(w)
    z_start(0)
    own_z = pltpu.make_async_copy(zt_s.at[pl.ds(row * cols, cols)], zr_s.at[row], loc_sem.at[0])
    own_z.start()
    for w in range(1, nt):
        make_bias(w)
    for w in range(1, nt):
        g_start(w)
    for copy in small[3:]:
        copy.wait()

    for idx, w in enumerate((wq_ref, wv_ref, wg_ref, wo_ref)):
        wt_s[idx] = w[...].astype(f32).T.astype(bf16)
    src_id = lax.broadcasted_iota(jnp.int32, (chan, 128), 0)
    dst_id = lax.broadcasted_iota(jnp.int32, (chan, 128), 1)
    for h in range(heads):
        pick = ((src_id == h * hd + dst_id % hd) & (dst_id < 3 * hd)).astype(f32).astype(bf16)
        wk_s[:, h * 128:(h + 1) * 128] = jnp.dot(wk_ref[...], pick, preferred_element_type=f32).astype(bf16)
    kept = jnp.sum(mask_ref[...].reshape(1, n), axis=1, keepdims=True)
    lane = lax.broadcasted_iota(jnp.int32, (sub, 128), 1)

    def join(pieces, w, half, oz, oy):
        for hh in range(2):
            for t in range(3):
                cut = block - 32 * t
                first, second = pieces(t, hh).astype(f32), pieces(t + 1, hh).astype(f32)
                piece = jnp.where(lane < cut, pltpu.roll(first, (128 - 32 * t) % 128, 1), pltpu.roll(second, cut, 1))
                bias_s[core, w, half, oz, oy, hh, :, t * 128:(t + 1) * 128] = piece.astype(bf16)

    def assemble_wide():
        wait_bytes(ga_s.at[pl.ds(0, 4 * rows - 1)], a_recv.at[0])
        for half in range(2):
            for pos in range(RING):
                oz, oy = (zc, pos) if half == 0 else (pos, yc)
                join(lambda t, hh: ga_s[half * 16 + pos * RING + t, hh], 0, half, oz, oy)

    def assemble(w):
        gb_s[w - 1, 0] = bt_s[core, w]
        wait_bytes(gb_s.at[w - 1, pl.ds(0, rows - 1)], g_recv.at[w - 1])
        for half in range(2):
            join(lambda t, hh: gb_s[w - 1, (row - half * 4 - t + rows) % rows, hh], w, half, zc, yc)

    def near_copy(w, half, d):
        blk = bias_s.at[core, w, half, zc, yc]
        return pltpu.make_async_remote_copy(src_ref=blk, dst_ref=blk, send_sem=p_send.at[0], recv_sem=p_near.at[w - 1, half],
                                            device_id=plane_peer(half == 0, d), device_id_type=MESH)

    def far_copy(w, half, d):
        blk = bias_s.at[core, w, half, zc] if half == 0 else bias_s.at[core, w, half, :, yc]
        return pltpu.make_async_remote_copy(src_ref=blk, dst_ref=blk, send_sem=p_send.at[1], recv_sem=p_far.at[w, half, d],
                                            device_id=plane_peer(half == 1, d), device_id_type=MESH)

    def pair_copy(w, half, d):
        if half == 0:
            blk = bias_s.at[core, w, half, (zc - d + RING) % RING]
        else:
            blk = bias_s.at[core, w, half, :, (yc - d + RING) % RING]
        return pltpu.make_async_remote_copy(src_ref=blk, dst_ref=blk, send_sem=d_send.at[0], recv_sem=d_recv.at[w],
                                            device_id=dev(col, row + 1 - 2 * core), device_id_type=MESH)

    def near_open(w):
        for d in (2, 1, 3):
            for half in range(2):
                near_copy(w, half, d).start()

    def near_close(w):
        for half in range(2):
            wait_bytes(bias_s.at[0, w, half, 0, pl.ds(0, RING - 1)], p_near.at[w - 1, half])

    def far_open(w):
        for d in (1, 3, 2):
            for half in range(2):
                far_copy(w, half, d).start()
        for half in range(2):
            pair_copy(w, half, 0).start()

    def far_close(w):
        for e in (1, 3, 2):
            for half in range(2):
                wait_bytes(bias_s.at[0, w, half, 0], p_far.at[w, half, e])
                pair_copy(w, half, e).start()

    def project(ck):
        wait_bytes(zr_s.at[pl.ds(0, rows - 1), pl.ds(0, 2)], z_recv.at[ck])

        @pl.loop(0, 2)
        def _(jj):
            j = 2 * ck + jj
            a = layer_norm(zr_s[:, j].astype(f32).reshape(n, chan), gamma, beta)
            keys = jnp.dot(a, wk_s[...], preferred_element_type=f32).astype(bf16)
            for h in range(heads):
                k_s[j, h] = keys[:, h * 128:(h + 1) * 128]
            vt_s[j] = lax.dot_general(wt_s[1], a, NT, preferred_element_type=f32).astype(bf16)
            zero = jnp.zeros((hd, TILE), bf16)
            for it in range(nt):
                aq = a.reshape(n // width, nt, sub, chan)[:, it].reshape(TILE, chan)
                gate_s[j, it] = jax.nn.sigmoid(lax.dot_general(wt_s[2], aq, NT, preferred_element_type=f32))
                qt = (lax.dot_general(wt_s[0], aq, NT, preferred_element_type=f32) * (1.0 / math.sqrt(hd))).astype(bf16)
                scaled = qt.astype(f32) * LOG2E
                top = scaled.astype(bf16)
                rest = scaled - top.astype(f32)
                mid = rest.astype(bf16)
                low = (rest - mid.astype(f32)).astype(bf16)
                for h in range(heads):
                    own = slice(h * hd, (h + 1) * hd)
                    qt_s[j, it, h] = jnp.concatenate([top[own], mid[own], low[own], zero], axis=0)

    eye = (lax.broadcasted_iota(jnp.int32, (128, 128), 0) == lax.broadcasted_iota(jnp.int32, (128, 128), 1)).astype(f32).astype(bf16)
    key = lax.broadcasted_iota(jnp.int32, (128, TILE), 0)

    def expand_bias(w):
        @pl.loop(0, 2)
        def _(ch):
            for hh in range(2):
                for half in range(2):
                    val = bias_s[ch, w, half, :, :, hh].reshape(TILE, n // 2)
                    for kt in range(3):
                        lo = half * (n // 2) + kt * 128
                        out = lax.dot_general(eye, val[:, kt * 128:(kt + 1) * 128], NT, preferred_element_type=f32)
                        biasf_s[2 * ch + hh, pl.ds(lo, 128), :] = (out + jnp.where(key < kept - lo, 0.0, MASK_FILL)) * LOG2E

    chunk = 128

    def fold(x, op):
        return op(x.reshape(x.shape[0] // 8, 8, TILE), axis=0)

    def logits(w, j, h, s_ref, m_ref):
        qt = qt_s[j, w, h]
        top = None
        for lo in range(0, n, chunk):
            s = jnp.dot(k_s[j, h, lo:lo + chunk, :], qt, preferred_element_type=f32) + biasf_s[h, lo:lo + chunk, :]
            s_ref[lo:lo + chunk, :] = s
            part = fold(s, jnp.max)
            top = part if top is None else jnp.maximum(top, part)
        m_ref[...] = top

    def finish_tile(w, j, h, s_ref, m_ref):
        top = jnp.max(m_ref[...], axis=0, keepdims=True)
        rows_h = pl.ds(pl.multiple_of(h * hd, hd), hd)
        total, o = None, None
        for lo in range(0, n, chunk):
            p = jnp.exp2(s_ref[lo:lo + chunk, :] - top)
            part = fold(p, jnp.sum)
            total = part if total is None else total + part
            prod = jnp.dot(vt_s[j, rows_h, lo:lo + chunk], p.astype(bf16), preferred_element_type=f32)
            o = prod if o is None else o + prod
        o_s[j, rows_h, :] = o / jnp.sum(total, axis=0, keepdims=True)

    def out_copy(w, j, d):
        peer = (row + d) % rows
        return pltpu.make_async_remote_copy(src_ref=res_s.at[w, j, peer], dst_ref=out_ref.at[row * cols + j, :, w], send_sem=o_send.at[0],
                                            recv_sem=o_recv.at[0], device_id=dev(col, peer), device_id_type=MESH)

    def finish_column(w, j):
        gated = (gate_s[j, w] * o_s[j]).astype(bf16)
        update = jnp.dot(wt_s[3], gated, preferred_element_type=f32)
        res = zr_s[:, j, :, w].astype(f32).reshape(TILE, chan) + update.T
        res_s[w, j] = res.astype(bf16).reshape(rows, 2, sub, chan)

    def send_column(w, j):
        for d in range(1, rows):
            out_copy(w, j, d).start()
        pltpu.make_async_copy(res_s.at[w, j, row], out_ref.at[row * cols + j, :, w], loc_sem.at[1]).start()

    def column(w, j, prev):
        if prev is not None:
            finish_column(*prev)
        for h in range(heads):
            here, there = ((s_a, m_a), (s_b, m_b)) if h % 2 == 0 else ((s_b, m_b), (s_a, m_a))
            if h < heads - 1:
                logits(w, j, h + 1, *there)
            else:
                logits(w, jnp.minimum(j + 1, cols - 1), 0, *there)
            finish_tile(w, j, h, *here)
        if prev is not None:
            send_column(*prev)

    def attend(w, j_lo, j_hi):
        @pl.loop(j_lo, j_hi)
        def _(j):
            column(w, j, (w, j - 1))

    def begin(w):
        wait_bytes(bias_s.at[0, w], d_recv.at[w])
        expand_bias(w)
        logits(w, 0, 0, s_a, m_a)

    last = cols - 1
    assemble_wide()
    far_open(0)
    z_start(1)
    z_start(2)
    for w in range(1, nt):
        assemble(w)
        near_open(w)
    own_z.wait()
    project(0)
    far_close(0)
    near_close(1)
    far_open(1)
    project(1)
    begin(0)
    column(0, 0, None)
    attend(0, 1, 4)
    far_close(1)
    near_close(2)
    far_open(2)
    project(2)
    logits(0, 4, 0, s_a, m_a)
    attend(0, 4, cols)
    begin(1)
    column(1, 0, (0, last))
    attend(1, 1, 3)
    far_close(2)
    attend(1, 3, cols)
    begin(2)
    column(2, 0, (1, last))
    attend(2, 1, cols)
    finish_column(2, last)
    send_column(2, last)

    wait_bytes(ga_s.at[pl.ds(0, 4 * rows - 1)], a_send.at[0])
    wait_bytes(gb_s.at[:, pl.ds(0, rows - 1)], g_send.at[0])
    wait_bytes(zr_s.at[pl.ds(0, rows - 1)], z_send.at[0])
    wait_bytes(bias_s.at[0, pl.ds(1, nt - 1), :, 0, pl.ds(0, RING - 1)], p_send.at[0])
    wait_bytes(bias_s.at[0, :, :, pl.ds(0, RING - 1)], p_send.at[1])
    wait_bytes(bias_s.at[0], d_send.at[0])
    wait_bytes(res_s.at[:, :, pl.ds(0, 1)], loc_sem.at[1])
    wait_bytes(res_s.at[:, :, pl.ds(0, rows - 1)], o_send.at[0])
    wait_bytes(res_s.at[:, :, pl.ds(0, rows - 1)], o_recv.at[0])


def solution(mesh):
    rows = mesh.shape['row']

    def body(pair_tile, res_mask, ln_gamma, ln_beta, w_q, w_k, w_v, w_b, w_g, w_o):
        block, width, chan = pair_tile.shape
        heads = w_b.shape[1]
        n = block * rows
        cols = width // rows
        bf16, f32 = jnp.bfloat16, jnp.float32
        nt = n // TILE
        sub = width // nt
        V = lambda *s, dt=bf16: pltpu.VMEM(s, dt)
        D = lambda *s: pltpu.SemaphoreType.DMA(s)
        out = pl.pallas_call(
            triangle_kernel,
            out_shape=jax.ShapeDtypeStruct((width, 2, nt, sub, chan), bf16),
            in_specs=[pl.BlockSpec(memory_space=pl.ANY)] * 10,
            out_specs=pl.BlockSpec(memory_space=pl.ANY),
            scratch_shapes=[V(block, width, chan), V(n, dt=jnp.int32), V(1, chan, dt=f32), V(1, chan, dt=f32), V(chan, chan), V(chan, chan),
                            V(chan, chan), V(heads, chan), V(chan, chan), V(chan, chan),
                            V(nt, block * sub, chan, dt=f32), V(block * sub, chan, dt=f32), V(width, 2, nt, sub, chan),
                            V(rows, cols, 2, nt, sub, chan), V(heads, sub, 128, dt=f32), V(2, nt, 2, sub, 128),
                            V(4 * rows, 2, sub, 128),
                            V(nt - 1, rows, 2, sub, 128), V(2, nt, 2, RING, RING, 2, sub, n // 2), V(heads, n, TILE, dt=f32),
                            V(4, chan, chan), V(chan, heads * 128), V(cols, nt, chan, TILE, dt=f32), V(cols, heads, n, 128), V(cols, chan, n),
                            V(cols, nt, heads, 128, TILE), V(n, TILE, dt=f32), V(n, TILE, dt=f32), V(8, TILE, dt=f32), V(8, TILE, dt=f32),
                            V(cols, chan, TILE, dt=f32), V(nt, cols, rows, 2, sub, chan),
                            D(1), D(1), D(1), D(nt - 1), D(1), D(cols // 2), D(2), D(nt - 1, 2), D(nt, 2, RING), D(1), D(nt), D(1), D(1), D(2), D(nt), D(9)],
            compiler_params=pltpu.CompilerParams(vmem_limit_bytes=60000 * 1024, collective_id=0,
                                                 has_side_effects=True),
            name='triangle',
        )(pair_tile, res_mask, ln_gamma.reshape(1, chan), ln_beta.reshape(1, chan), w_q, w_k, w_v, w_b.T, w_g, w_o)
        return jnp.transpose(out.reshape(width, block, chan), (1, 0, 2))

    tile_spec = P(('data', 'row'), 'col', None)
    return jax.shard_map(body, mesh=mesh, in_specs=(tile_spec, P('data'), P(), P(), P(), P(), P(), P(), P(), P()), out_specs=tile_spec, check_vma=False)
```

```python
import math
import jax
import jax.numpy as jnp
from jax import lax
from jax.experimental import pallas as pl
from jax.experimental.pallas import tpu as pltpu
from jax.sharding import PartitionSpec as P

LN_EPS = 1e-5
MASK_FILL = -1e9
LOG2E = math.log2(math.e)
NT = (((1,), (1,)), ((), ()))
MESH = pl.DeviceIdType.MESH
TILE = 256
RING = 4


def layer_norm(z, gamma, beta):
    mean = jnp.mean(z, axis=-1, keepdims=True)
    centred = z - mean
    variance = jnp.mean(centred * centred, axis=-1, keepdims=True)
    return (centred * lax.rsqrt(variance + LN_EPS) * gamma + beta).astype(jnp.bfloat16)


def triangle_kernel(z_hbm, mask_hbm, gamma_hbm, beta_hbm, wq_hbm, wk_hbm, wv_hbm, wb_hbm, wg_hbm, wo_hbm, out_ref,
                    z_ref, mask_ref, gamma_ref, beta_ref, wq_ref, wk_ref, wv_ref, wb_ref, wg_ref, wo_ref,
                    zf_s, af_s, zt_s, zr_s, bst_s, bt_s, gb_s, bias_s, biasf_s, wt_s, wk_s, gate_s, k_s, vt_s, qt_s, s_a, s_b, m_a, m_b, o_s, res_s,
                    g_send, g_recv, z_send, z_recv, p_send, p_near, p_far, d_send, d_recv, o_send, o_recv, loc_sem, z_sem, in_sem):
    f32, bf16 = jnp.float32, jnp.bfloat16
    data, col, row = lax.axis_index('data'), lax.axis_index('col'), lax.axis_index('row')
    rows, cols, chan = zr_s.shape[0], zr_s.shape[1], zr_s.shape[-1]
    width = rows * cols
    block = z_ref.shape[0]
    n = rows * block
    heads = wb_ref.shape[0]
    hd = chan // heads
    nt = n // TILE
    sub = width // nt
    core = row % 2
    zc, yc = col // RING, col % RING

    def dev(c, r):
        return (data, c, r)

    def row_peer(d):
        return dev(col, (row + d) % rows)

    def plane_peer(along_y, d):
        if along_y:
            return dev(zc * RING + (yc + d) % RING, row)
        return dev((zc + d) % RING * RING + yc, row)

    def load_z(w):
        piece = (slice(None), pl.ds(w * sub, sub))
        return pltpu.make_async_copy(z_hbm.at[piece], z_ref.at[piece], z_sem.at[w])

    small = [pltpu.make_async_copy(src, dst, in_sem.at[idx]) for idx, (src, dst) in enumerate((
        (gamma_hbm, gamma_ref), (beta_hbm, beta_ref), (wb_hbm, wb_ref), (mask_hbm, mask_ref), (wq_hbm, wq_ref), (wk_hbm, wk_ref),
        (wv_hbm, wv_ref), (wg_hbm, wg_ref), (wo_hbm, wo_ref)))]
    load_z(0).start()
    for copy in small:
        copy.start()
    for w in range(1, nt):
        load_z(w).start()
    barrier = pltpu.get_barrier_semaphore()
    for d in range(1, rows):
        pl.semaphore_signal(barrier, inc=1, device_id=row_peer(d), device_id_type=MESH)
    for along_y in (True, False):
        for d in range(1, RING):
            pl.semaphore_signal(barrier, inc=1, device_id=plane_peer(along_y, d), device_id_type=MESH)

    for copy in small[:3]:
        copy.wait()
    gamma, beta = gamma_ref[...], beta_ref[...]
    wbt = wb_ref[...]
    bst_s[...] = jnp.zeros_like(bst_s)

    def make_bias(w):
        half_rows = block // 2
        if w == 0:
            load_z(w).wait()

        @pl.loop(0, 2)
        def _(c):
            z = z_ref[pl.ds(c * half_rows, half_rows), w * sub:(w + 1) * sub, :].astype(f32).reshape(half_rows * sub, chan)
            here = pl.ds(pl.multiple_of(c * half_rows * sub, half_rows * sub), half_rows * sub)
            if w == 0:
                zf_s[0, here, :] = z
            af_s[here, :] = layer_norm(z, gamma, beta).astype(f32)

        for t in range(sub):
            b = lax.dot_general(wbt, af_s[pl.ds(t, block, stride=sub), :].astype(bf16), NT, preferred_element_type=f32)
            for h in range(heads):
                bst_s[h, pl.ds(t, 1), :block] = b[h:h + 1]
        for h in range(heads):
            bt_s[h // 2, w, h % 2] = bst_s[h].astype(bf16)

    def transpose_z(w):
        if w > 0:
            load_z(w).wait()
            zf_s[w] = z_ref[:, w * sub:(w + 1) * sub, :].astype(f32).reshape(block * sub, chan)
        for t in range(sub):
            col_z = zf_s[w, pl.ds(t, block, stride=sub), :].astype(bf16)
            zt_s[w * sub + t] = col_z.reshape(2, nt, sub, chan)

    def wait_bytes(ref, sem):
        pltpu.make_async_copy(ref, ref, sem).wait()

    def g_copy(w, d):
        peer = (row + d) % rows
        return pltpu.make_async_remote_copy(src_ref=bt_s.at[peer % 2, w], dst_ref=gb_s.at[w, d], send_sem=g_send.at[0], recv_sem=g_recv.at[w],
                                            device_id=dev(col, peer), device_id_type=MESH)

    def g_start(w):
        for d in (4, 3, 5, 2, 6, 7, 1):
            g_copy(w, d).start()

    def z_start(ck):
        for d in range(1, rows):
            z_copy(d, ck).start()

    def z_copy(d, ck):
        peer = (row + d) % rows
        return pltpu.make_async_remote_copy(src_ref=zt_s.at[pl.ds(peer * cols + 2 * ck, 2)], dst_ref=zr_s.at[row, pl.ds(2 * ck, 2)],
                                            send_sem=z_send.at[0], recv_sem=z_recv.at[ck], device_id=dev(col, peer), device_id_type=MESH)

    make_bias(0)
    pl.semaphore_wait(barrier, rows - 1 + 2 * (RING - 1))
    g_start(0)
    for w in range(nt):
        transpose_z(w)
    z_start(0)
    own_z = pltpu.make_async_copy(zt_s.at[pl.ds(row * cols, cols)], zr_s.at[row], loc_sem.at[0])
    own_z.start()
    for w in range(1, nt):
        make_bias(w)
        g_start(w)
        z_start(w)
    for copy in small[3:]:
        copy.wait()

    for idx, w in enumerate((wq_ref, wv_ref, wg_ref, wo_ref)):
        wt_s[idx] = w[...].astype(f32).T.astype(bf16)
    src_id = lax.broadcasted_iota(jnp.int32, (chan, 128), 0)
    dst_id = lax.broadcasted_iota(jnp.int32, (chan, 128), 1)
    for h in range(heads):
        pick = ((src_id == h * hd + dst_id % hd) & (dst_id < 3 * hd)).astype(f32).astype(bf16)
        wk_s[:, h * 128:(h + 1) * 128] = jnp.dot(wk_ref[...], pick, preferred_element_type=f32).astype(bf16)
    kept = jnp.sum(mask_ref[...].reshape(1, n), axis=1, keepdims=True)
    lane = lax.broadcasted_iota(jnp.int32, (sub, 128), 1)

    def assemble(w):
        gb_s[w, 0] = bt_s[core, w]
        wait_bytes(gb_s.at[w, pl.ds(0, rows - 1)], g_recv.at[w])
        for hh in range(2):
            for half in range(2):
                for t in range(3):
                    lo = half * 4 + t
                    first = gb_s[w, (row - lo + rows) % rows, hh].astype(f32)
                    second = gb_s[w, (row - lo - 1 + rows) % rows, hh].astype(f32)
                    cut = block - 32 * t
                    piece = jnp.where(lane < cut, pltpu.roll(first, (128 - 32 * t) % 128, 1), pltpu.roll(second, cut, 1))
                    bias_s[core, w, half, zc, yc, hh, :, t * 128:(t + 1) * 128] = piece.astype(bf16)

    def plane_copy(w, half, first, origin, d):
        along_y = (half == 0) == first
        oz, oy = (zc, (yc + origin) % RING) if half == 0 else ((zc + origin) % RING, yc)
        blk = bias_s.at[core, w, half, oz, oy]
        recv = p_near.at[w, half] if first else p_far.at[w, half, d]
        return pltpu.make_async_remote_copy(src_ref=blk, dst_ref=blk, send_sem=p_send.at[0 if first else 1], recv_sem=recv,
                                            device_id=plane_peer(along_y, d), device_id_type=MESH)

    def pair_copy(w, half, d):
        if half == 0:
            blk = bias_s.at[core, w, half, (zc - d + RING) % RING]
        else:
            blk = bias_s.at[core, w, half, :, (yc - d + RING) % RING]
        return pltpu.make_async_remote_copy(src_ref=blk, dst_ref=blk, send_sem=d_send.at[0], recv_sem=d_recv.at[w],
                                            device_id=dev(col, row + 1 - 2 * core), device_id_type=MESH)

    def plane_open(w):
        for first in (True, False):
            for half in range(2):
                for d in (2, 1, 3):
                    plane_copy(w, half, first, 0, d).start()

    def plane_forward(w):
        for half in range(2):
            wait_bytes(bias_s.at[0, w, half, 0, pl.ds(0, RING - 1)], p_near.at[w, half])
            for origin in range(1, RING):
                for e in (2, 1, 3):
                    plane_copy(w, half, False, origin, e).start()
            pair_copy(w, half, 0).start()

    def plane_close(w):
        for e in (1, 3, 2):
            for half in range(2):
                wait_bytes(bias_s.at[0, w, half, 0], p_far.at[w, half, e])
                pair_copy(w, half, e).start()

    def project(ck):
        wait_bytes(zr_s.at[pl.ds(0, rows - 1), pl.ds(0, 2)], z_recv.at[ck])

        @pl.loop(0, 2)
        def _(jj):
            j = 2 * ck + jj
            a = layer_norm(zr_s[:, j].astype(f32).reshape(n, chan), gamma, beta)
            keys = jnp.dot(a, wk_s[...], preferred_element_type=f32).astype(bf16)
            for h in range(heads):
                k_s[j, h] = keys[:, h * 128:(h + 1) * 128]
            vt_s[j] = lax.dot_general(wt_s[1], a, NT, preferred_element_type=f32).astype(bf16)
            zero = jnp.zeros((hd, TILE), bf16)
            for it in range(nt):
                aq = a.reshape(n // width, nt, sub, chan)[:, it].reshape(TILE, chan)
                gate_s[j, it] = jax.nn.sigmoid(lax.dot_general(wt_s[2], aq, NT, preferred_element_type=f32))
                qt = (lax.dot_general(wt_s[0], aq, NT, preferred_element_type=f32) * (1.0 / math.sqrt(hd))).astype(bf16)
                scaled = qt.astype(f32) * LOG2E
                top = scaled.astype(bf16)
                rest = scaled - top.astype(f32)
                mid = rest.astype(bf16)
                low = (rest - mid.astype(f32)).astype(bf16)
                for h in range(heads):
                    own = slice(h * hd, (h + 1) * hd)
                    qt_s[j, it, h] = jnp.concatenate([top[own], mid[own], low[own], zero], axis=0)

    eye = (lax.broadcasted_iota(jnp.int32, (128, 128), 0) == lax.broadcasted_iota(jnp.int32, (128, 128), 1)).astype(f32).astype(bf16)
    key = lax.broadcasted_iota(jnp.int32, (128, TILE), 0)

    def expand_bias(w):
        @pl.loop(0, 2)
        def _(ch):
            for hh in range(2):
                for half in range(2):
                    val = bias_s[ch, w, half, :, :, hh].reshape(TILE, n // 2)
                    for kt in range(3):
                        lo = half * (n // 2) + kt * 128
                        out = lax.dot_general(eye, val[:, kt * 128:(kt + 1) * 128], NT, preferred_element_type=f32)
                        biasf_s[2 * ch + hh, pl.ds(lo, 128), :] = (out + jnp.where(key < kept - lo, 0.0, MASK_FILL)) * LOG2E

    chunk = 128

    def fold(x, op):
        return op(x.reshape(x.shape[0] // 8, 8, TILE), axis=0)

    def logits(w, j, h, s_ref, m_ref):
        qt = qt_s[j, w, h]
        top = None
        for lo in range(0, n, chunk):
            s = jnp.dot(k_s[j, h, lo:lo + chunk, :], qt, preferred_element_type=f32) + biasf_s[h, lo:lo + chunk, :]
            s_ref[lo:lo + chunk, :] = s
            part = fold(s, jnp.max)
            top = part if top is None else jnp.maximum(top, part)
        m_ref[...] = top

    def finish_tile(w, j, h, s_ref, m_ref):
        top = jnp.max(m_ref[...], axis=0, keepdims=True)
        rows_h = pl.ds(pl.multiple_of(h * hd, hd), hd)
        total, o = None, None
        for lo in range(0, n, chunk):
            p = jnp.exp2(s_ref[lo:lo + chunk, :] - top)
            part = fold(p, jnp.sum)
            total = part if total is None else total + part
            prod = jnp.dot(vt_s[j, rows_h, lo:lo + chunk], p.astype(bf16), preferred_element_type=f32)
            o = prod if o is None else o + prod
        o_s[j, rows_h, :] = o / jnp.sum(total, axis=0, keepdims=True)

    def out_copy(w, j, d):
        peer = (row + d) % rows
        return pltpu.make_async_remote_copy(src_ref=res_s.at[w, j, peer], dst_ref=out_ref.at[row * cols + j, :, w], send_sem=o_send.at[0],
                                            recv_sem=o_recv.at[0], device_id=dev(col, peer), device_id_type=MESH)

    def finish_column(w, j):
        gated = (gate_s[j, w] * o_s[j]).astype(bf16)
        update = jnp.dot(wt_s[3], gated, preferred_element_type=f32)
        res = zr_s[:, j, :, w].astype(f32).reshape(TILE, chan) + update.T
        res_s[w, j] = res.astype(bf16).reshape(rows, 2, sub, chan)

    def send_column(w, j):
        for d in range(1, rows):
            out_copy(w, j, d).start()
        pltpu.make_async_copy(res_s.at[w, j, row], out_ref.at[row * cols + j, :, w], loc_sem.at[1]).start()

    def column(w, j, prev):
        if prev is not None:
            finish_column(*prev)
        for h in range(heads):
            here, there = ((s_a, m_a), (s_b, m_b)) if h % 2 == 0 else ((s_b, m_b), (s_a, m_a))
            if h < heads - 1:
                logits(w, j, h + 1, *there)
            else:
                logits(w, jnp.minimum(j + 1, cols - 1), 0, *there)
            finish_tile(w, j, h, *here)
        if prev is not None:
            send_column(*prev)

    def attend(w, j_lo, j_hi):
        @pl.loop(j_lo, j_hi)
        def _(j):
            column(w, j, (w, j - 1))

    def begin(w):
        wait_bytes(bias_s.at[0, w], d_recv.at[w])
        expand_bias(w)
        logits(w, 0, 0, s_a, m_a)

    last = cols - 1
    assemble(0)
    plane_open(0)
    plane_forward(0)
    assemble(1)
    plane_open(1)
    own_z.wait()
    project(0)
    project(1)
    plane_close(0)
    plane_forward(1)
    assemble(2)
    plane_open(2)
    project(2)
    begin(0)
    column(0, 0, None)
    attend(0, 1, 3)
    plane_close(1)
    plane_forward(2)
    attend(0, 3, cols)
    begin(1)
    column(1, 0, (0, last))
    attend(1, 1, 3)
    plane_close(2)
    attend(1, 3, cols)
    begin(2)
    column(2, 0, (1, last))
    attend(2, 1, cols)
    finish_column(2, last)
    send_column(2, last)

    wait_bytes(gb_s.at[:, pl.ds(0, rows - 1)], g_send.at[0])
    wait_bytes(zr_s.at[pl.ds(0, rows - 1)], z_send.at[0])
    wait_bytes(bias_s.at[0, :, :, 0, pl.ds(0, RING - 1)], p_send.at[0])
    wait_bytes(bias_s.at[0, :, :, pl.ds(0, RING - 1)], p_send.at[1])
    wait_bytes(bias_s.at[0], d_send.at[0])
    wait_bytes(res_s.at[:, :, pl.ds(0, 1)], loc_sem.at[1])
    wait_bytes(res_s.at[:, :, pl.ds(0, rows - 1)], o_send.at[0])
    wait_bytes(res_s.at[:, :, pl.ds(0, rows - 1)], o_recv.at[0])


def solution(mesh):
    rows = mesh.shape['row']

    def body(pair_tile, res_mask, ln_gamma, ln_beta, w_q, w_k, w_v, w_b, w_g, w_o):
        block, width, chan = pair_tile.shape
        heads = w_b.shape[1]
        n = block * rows
        cols = width // rows
        bf16, f32 = jnp.bfloat16, jnp.float32
        nt = n // TILE
        sub = width // nt
        V = lambda *s, dt=bf16: pltpu.VMEM(s, dt)
        D = lambda *s: pltpu.SemaphoreType.DMA(s)
        out = pl.pallas_call(
            triangle_kernel,
            out_shape=pltpu.VMEM((width, 2, nt, sub, chan), bf16),
            in_specs=[pl.BlockSpec(memory_space=pl.ANY)] * 10,
            out_specs=pl.BlockSpec(memory_space=pltpu.VMEM),
            scratch_shapes=[V(block, width, chan), V(n, dt=jnp.int32), V(1, chan, dt=f32), V(1, chan, dt=f32), V(chan, chan), V(chan, chan),
                            V(chan, chan), V(heads, chan), V(chan, chan), V(chan, chan),
                            V(nt, block * sub, chan, dt=f32), V(block * sub, chan, dt=f32), V(width, 2, nt, sub, chan),
                            V(rows, cols, 2, nt, sub, chan), V(heads, sub, 128, dt=f32), V(2, nt, 2, sub, 128),
                            V(nt, rows, 2, sub, 128), V(2, nt, 2, RING, RING, 2, sub, n // 2), V(heads, n, TILE, dt=f32),
                            V(4, chan, chan), V(chan, heads * 128), V(cols, nt, chan, TILE, dt=f32), V(cols, heads, n, 128), V(cols, chan, n),
                            V(cols, nt, heads, 128, TILE), V(n, TILE, dt=f32), V(n, TILE, dt=f32), V(8, TILE, dt=f32), V(8, TILE, dt=f32),
                            V(cols, chan, TILE, dt=f32), V(nt, cols, rows, 2, sub, chan),
                            D(1), D(nt), D(1), D(cols // 2), D(2), D(nt, 2), D(nt, 2, RING), D(1), D(nt), D(1), D(1), D(2), D(nt), D(9)],
            compiler_params=pltpu.CompilerParams(vmem_limit_bytes=65_700_000, collective_id=0,
                                                 has_side_effects=True),
            name='triangle',
        )(pair_tile, res_mask, ln_gamma.reshape(1, chan), ln_beta.reshape(1, chan), w_q, w_k, w_v, w_b.T, w_g, w_o)
        return jnp.transpose(out.reshape(width, block, chan), (1, 0, 2))

    tile_spec = P(('data', 'row'), 'col', None)
    return jax.shard_map(body, mesh=mesh, in_specs=(tile_spec, P('data'), P(), P(), P(), P(), P(), P(), P(), P()), out_specs=tile_spec, check_vma=False)
```

```python
import math
import jax
import jax.numpy as jnp
from jax import lax
from jax.experimental import pallas as pl
from jax.experimental.pallas import tpu as pltpu
from jax.sharding import PartitionSpec as P

LN_EPS = 1e-5
MASK_FILL = -1e9
LOG2E = math.log2(math.e)
NT = (((1,), (1,)), ((), ()))
MESH = pl.DeviceIdType.MESH
TILE = 256
RING = 4


def layer_norm(z, gamma, beta):
    mean = jnp.mean(z, axis=-1, keepdims=True)
    centred = z - mean
    variance = jnp.mean(centred * centred, axis=-1, keepdims=True)
    return (centred * lax.rsqrt(variance + LN_EPS) * gamma + beta).astype(jnp.bfloat16)


def triangle_kernel(z_hbm, mask_hbm, gamma_hbm, beta_hbm, wq_hbm, wk_hbm, wv_hbm, wb_hbm, wg_hbm, wo_hbm, out_ref,
                    z_ref, mask_ref, gamma_ref, beta_ref, wq_ref, wk_ref, wv_ref, wb_ref, wg_ref, wo_ref,
                    fill_s, zf_s, af_s, zt_s, zr_s, bst_s, bt_s, gb_s, bias_s, biasf_s, wt_s, wk_s, gate_s, k_s, vt_s, qt_s, s_a, s_b, m_a, m_b, o_s, res_s,
                    g_send, g_recv, z_send, z_recv, p_send, p_near, p_far, d_send, d_recv, o_send, o_recv, loc_sem, z_sem, in_sem):
    f32, bf16 = jnp.float32, jnp.bfloat16
    data, col, row = lax.axis_index('data'), lax.axis_index('col'), lax.axis_index('row')
    rows, cols, chan = zr_s.shape[0], zr_s.shape[1], zr_s.shape[-1]
    width = rows * cols
    block = z_ref.shape[0]
    n = rows * block
    heads = wb_ref.shape[0]
    hd = chan // heads
    nt = n // TILE
    sub = width // nt
    core = row % 2
    zc, yc = col // RING, col % RING

    def dev(c, r):
        return (data, c, r)

    def row_peer(d):
        return dev(col, (row + d) % rows)

    def plane_peer(along_y, d):
        if along_y:
            return dev(zc * RING + (yc + d) % RING, row)
        return dev((zc + d) % RING * RING + yc, row)

    def load_z(w):
        piece = (slice(None), pl.ds(w * sub, sub))
        return pltpu.make_async_copy(z_hbm.at[piece], z_ref.at[piece], z_sem.at[w])

    small = [pltpu.make_async_copy(src, dst, in_sem.at[idx]) for idx, (src, dst) in enumerate((
        (gamma_hbm, gamma_ref), (beta_hbm, beta_ref), (wb_hbm, wb_ref), (mask_hbm, mask_ref), (wq_hbm, wq_ref), (wk_hbm, wk_ref),
        (wv_hbm, wv_ref), (wg_hbm, wg_ref), (wo_hbm, wo_ref)))]
    load_z(0).start()
    for copy in small:
        copy.start()
    for w in range(1, nt):
        load_z(w).start()
    barrier = pltpu.get_barrier_semaphore()
    for d in range(1, rows):
        pl.semaphore_signal(barrier, inc=1, device_id=row_peer(d), device_id_type=MESH)
    for along_y in (True, False):
        for d in range(1, RING):
            pl.semaphore_signal(barrier, inc=1, device_id=plane_peer(along_y, d), device_id_type=MESH)

    for copy in small[:3]:
        copy.wait()
    gamma, beta = gamma_ref[...], beta_ref[...]
    wbt = wb_ref[...]
    bst_s[...] = jnp.zeros_like(bst_s)

    def make_bias(w):
        half_rows = block // 2
        if w == 0:
            load_z(w).wait()

        @pl.loop(0, 2)
        def _(c):
            z = z_ref[pl.ds(c * half_rows, half_rows), w * sub:(w + 1) * sub, :].astype(f32).reshape(half_rows * sub, chan)
            here = pl.ds(pl.multiple_of(c * half_rows * sub, half_rows * sub), half_rows * sub)
            if w == 0:
                zf_s[0, here, :] = z
            af_s[here, :] = layer_norm(z, gamma, beta).astype(f32)

        for t in range(sub):
            b = lax.dot_general(wbt, af_s[pl.ds(t, block, stride=sub), :].astype(bf16), NT, preferred_element_type=f32)
            for h in range(heads):
                bst_s[h, pl.ds(t, 1), :block] = b[h:h + 1]
        for h in range(heads):
            bt_s[h // 2, w, h % 2] = bst_s[h].astype(bf16)

    def transpose_z(w):
        if w > 0:
            load_z(w).wait()
            zf_s[w] = z_ref[:, w * sub:(w + 1) * sub, :].astype(f32).reshape(block * sub, chan)
        for t in range(sub):
            col_z = zf_s[w, pl.ds(t, block, stride=sub), :].astype(bf16)
            zt_s[w * sub + t] = col_z.reshape(2, nt, sub, chan)

    def wait_bytes(ref, sem):
        pltpu.make_async_copy(ref, ref, sem).wait()

    def g_copy(w, d):
        peer = (row + d) % rows
        return pltpu.make_async_remote_copy(src_ref=bt_s.at[peer % 2, w], dst_ref=gb_s.at[w, d], send_sem=g_send.at[0], recv_sem=g_recv.at[w],
                                            device_id=dev(col, peer), device_id_type=MESH)

    def g_start(w):
        for d in (4, 3, 5, 2, 6, 7, 1):
            g_copy(w, d).start()

    def z_start(ck):
        for d in range(1, rows):
            z_copy(d, ck).start()

    def z_copy(d, ck):
        peer = (row + d) % rows
        return pltpu.make_async_remote_copy(src_ref=zt_s.at[pl.ds(peer * cols + 2 * ck, 2)], dst_ref=zr_s.at[row, pl.ds(2 * ck, 2)],
                                            send_sem=z_send.at[0], recv_sem=z_recv.at[ck], device_id=dev(col, peer), device_id_type=MESH)

    make_bias(0)
    pl.semaphore_wait(barrier, rows - 1 + 2 * (RING - 1))
    g_start(0)
    for w in range(nt):
        transpose_z(w)
    z_start(0)
    own_z = pltpu.make_async_copy(zt_s.at[pl.ds(row * cols, cols)], zr_s.at[row], loc_sem.at[0])
    own_z.start()
    for w in range(1, nt):
        make_bias(w)
        g_start(w)
        z_start(w)
    for copy in small[3:]:
        copy.wait()

    for idx, w in enumerate((wq_ref, wv_ref, wg_ref, wo_ref)):
        wt_s[idx] = w[...].astype(f32).T.astype(bf16)
    src_id = lax.broadcasted_iota(jnp.int32, (chan, 128), 0)
    dst_id = lax.broadcasted_iota(jnp.int32, (chan, 128), 1)
    for h in range(heads):
        pick = ((src_id == h * hd + dst_id % hd) & (dst_id < 3 * hd)).astype(f32).astype(bf16)
        wk_s[:, h * 128:(h + 1) * 128] = jnp.dot(wk_ref[...], pick, preferred_element_type=f32).astype(bf16)
    kept = jnp.sum(mask_ref[...].reshape(1, n), axis=1, keepdims=True)
    fill_s[...] = jnp.where(lax.broadcasted_iota(jnp.int32, (n, TILE), 0) < kept, 0.0, MASK_FILL * LOG2E)
    lane = lax.broadcasted_iota(jnp.int32, (sub, 128), 1)

    def assemble(w):
        gb_s[w, 0] = bt_s[core, w]
        wait_bytes(gb_s.at[w, pl.ds(0, rows - 1)], g_recv.at[w])
        for hh in range(2):
            for half in range(2):
                for t in range(3):
                    lo = half * 4 + t
                    first = gb_s[w, (row - lo + rows) % rows, hh].astype(f32)
                    second = gb_s[w, (row - lo - 1 + rows) % rows, hh].astype(f32)
                    cut = block - 32 * t
                    piece = jnp.where(lane < cut, pltpu.roll(first, (128 - 32 * t) % 128, 1), pltpu.roll(second, cut, 1))
                    bias_s[core, w, half, zc, yc, hh, :, t * 128:(t + 1) * 128] = piece.astype(bf16)

    def plane_copy(w, half, first, origin, d):
        along_y = (half == 0) == first
        oz, oy = (zc, (yc + origin) % RING) if half == 0 else ((zc + origin) % RING, yc)
        blk = bias_s.at[core, w, half, oz, oy]
        recv = p_near.at[w, half] if first else p_far.at[w, half, d]
        return pltpu.make_async_remote_copy(src_ref=blk, dst_ref=blk, send_sem=p_send.at[0 if first else 1], recv_sem=recv,
                                            device_id=plane_peer(along_y, d), device_id_type=MESH)

    def pair_copy(w, half, d):
        if half == 0:
            blk = bias_s.at[core, w, half, (zc - d + RING) % RING]
        else:
            blk = bias_s.at[core, w, half, :, (yc - d + RING) % RING]
        return pltpu.make_async_remote_copy(src_ref=blk, dst_ref=blk, send_sem=d_send.at[0], recv_sem=d_recv.at[w],
                                            device_id=dev(col, row + 1 - 2 * core), device_id_type=MESH)

    def plane_open(w):
        for first in (True, False):
            for half in range(2):
                for d in (2, 1, 3):
                    plane_copy(w, half, first, 0, d).start()

    def plane_forward(w):
        for half in range(2):
            wait_bytes(bias_s.at[0, w, half, 0, pl.ds(0, RING - 1)], p_near.at[w, half])
            for origin in range(1, RING):
                for e in (2, 1, 3):
                    plane_copy(w, half, False, origin, e).start()
            pair_copy(w, half, 0).start()

    def plane_close(w):
        for e in (1, 3, 2):
            for half in range(2):
                wait_bytes(bias_s.at[0, w, half, 0], p_far.at[w, half, e])
                pair_copy(w, half, e).start()

    def project(ck):
        wait_bytes(zr_s.at[pl.ds(0, rows - 1), pl.ds(0, 2)], z_recv.at[ck])

        @pl.loop(0, 2)
        def _(jj):
            j = 2 * ck + jj
            a = layer_norm(zr_s[:, j].astype(f32).reshape(n, chan), gamma, beta)
            keys = jnp.dot(a, wk_s[...], preferred_element_type=f32).astype(bf16)
            for h in range(heads):
                k_s[j, h] = keys[:, h * 128:(h + 1) * 128]
            vt_s[j] = lax.dot_general(wt_s[1], a, NT, preferred_element_type=f32).astype(bf16)
            zero = jnp.zeros((hd, TILE), bf16)
            for it in range(nt):
                aq = a.reshape(n // width, nt, sub, chan)[:, it].reshape(TILE, chan)
                gate_s[j, it] = jax.nn.sigmoid(lax.dot_general(wt_s[2], aq, NT, preferred_element_type=f32))
                qt = (lax.dot_general(wt_s[0], aq, NT, preferred_element_type=f32) * (1.0 / math.sqrt(hd))).astype(bf16)
                scaled = qt.astype(f32) * LOG2E
                top = scaled.astype(bf16)
                rest = scaled - top.astype(f32)
                mid = rest.astype(bf16)
                low = (rest - mid.astype(f32)).astype(bf16)
                for h in range(heads):
                    own = slice(h * hd, (h + 1) * hd)
                    qt_s[j, it, h] = jnp.concatenate([top[own], mid[own], low[own], zero], axis=0)

    eye = (lax.broadcasted_iota(jnp.int32, (128, 128), 0) == lax.broadcasted_iota(jnp.int32, (128, 128), 1)).astype(f32).astype(bf16)

    def expand_bias(w):
        @pl.loop(0, 2)
        def _(ch):
            for hh in range(2):
                for half in range(2):
                    val = bias_s[ch, w, half, :, :, hh].reshape(TILE, n // 2)
                    for kt in range(3):
                        lo = half * (n // 2) + kt * 128
                        out = lax.dot_general(eye, val[:, kt * 128:(kt + 1) * 128], NT, preferred_element_type=f32)
                        biasf_s[2 * ch + hh, pl.ds(lo, 128), :] = out * LOG2E + fill_s[lo:lo + 128, :]

    chunk = 192

    def fold(x, op):
        return op(x.reshape(x.shape[0] // 8, 8, TILE), axis=0)

    def logits(w, j, h, s_ref, m_ref):
        qt = qt_s[j, w, h]
        top = None
        for lo in range(0, n, chunk):
            s = jnp.dot(k_s[j, h, lo:lo + chunk, :], qt, preferred_element_type=f32) + biasf_s[h, lo:lo + chunk, :]
            s_ref[lo:lo + chunk, :] = s
            part = fold(s, jnp.max)
            top = part if top is None else jnp.maximum(top, part)
        m_ref[...] = top

    def finish_tile(w, j, h, s_ref, m_ref):
        top = jnp.max(m_ref[...], axis=0, keepdims=True)
        rows_h = pl.ds(pl.multiple_of(h * hd, hd), hd)
        total, o = None, None
        for lo in range(0, n, 192):
            p = jnp.exp2(s_ref[lo:lo + 192, :] - top)
            part = fold(p, jnp.sum)
            total = part if total is None else total + part
            prod = jnp.dot(vt_s[j, rows_h, lo:lo + 192], p.astype(bf16), preferred_element_type=f32)
            o = prod if o is None else o + prod
        o_s[j, rows_h, :] = o / jnp.sum(total, axis=0, keepdims=True)

    def out_copy(w, j, d):
        peer = (row + d) % rows
        return pltpu.make_async_remote_copy(src_ref=res_s.at[w, j, peer], dst_ref=out_ref.at[row * cols + j, :, w], send_sem=o_send.at[0],
                                            recv_sem=o_recv.at[0], device_id=dev(col, peer), device_id_type=MESH)

    def finish_column(w, j):
        gated = (gate_s[j, w] * o_s[j]).astype(bf16)
        update = jnp.dot(wt_s[3], gated, preferred_element_type=f32)
        res = zr_s[:, j, :, w].astype(f32).reshape(TILE, chan) + update.T
        res_s[w, j] = res.astype(bf16).reshape(rows, 2, sub, chan)

    def send_column(w, j):
        for d in range(1, rows):
            out_copy(w, j, d).start()
        pltpu.make_async_copy(res_s.at[w, j, row], out_ref.at[row * cols + j, :, w], loc_sem.at[1]).start()

    def column(w, j, prev, more=True):
        if prev is not None:
            finish_column(*prev)
        for h in range(heads):
            here, there = ((s_a, m_a), (s_b, m_b)) if h % 2 == 0 else ((s_b, m_b), (s_a, m_a))
            if h < heads - 1:
                logits(w, j, h + 1, *there)
            elif more:
                logits(w, j + 1, 0, *there)
            finish_tile(w, j, h, *here)
        if prev is not None:
            send_column(*prev)

    def attend(w, j_lo, j_hi):
        @pl.loop(j_lo, j_hi)
        def _(j):
            column(w, j, (w, j - 1))

    def begin(w):
        wait_bytes(bias_s.at[0, w], d_recv.at[w])
        expand_bias(w)
        logits(w, 0, 0, s_a, m_a)

    last = cols - 1
    assemble(0)
    plane_open(0)
    plane_forward(0)
    assemble(1)
    plane_open(1)
    own_z.wait()
    project(0)
    project(1)
    plane_close(0)
    plane_forward(1)
    assemble(2)
    plane_open(2)
    project(2)
    begin(0)
    column(0, 0, None)
    attend(0, 1, 3)
    plane_close(1)
    plane_forward(2)
    attend(0, 3, last)
    column(0, last, (0, last - 1), False)
    begin(1)
    column(1, 0, (0, last))
    attend(1, 1, 3)
    plane_close(2)
    attend(1, 3, last)
    column(1, last, (1, last - 1), False)
    begin(2)
    column(2, 0, (1, last))
    attend(2, 1, last)
    column(2, last, (2, last - 1), False)
    finish_column(2, last)
    send_column(2, last)

    wait_bytes(gb_s.at[:, pl.ds(0, rows - 1)], g_send.at[0])
    wait_bytes(zr_s.at[pl.ds(0, rows - 1)], z_send.at[0])
    wait_bytes(bias_s.at[0, :, :, 0, pl.ds(0, RING - 1)], p_send.at[0])
    wait_bytes(bias_s.at[0, :, :, pl.ds(0, RING - 1)], p_send.at[1])
    wait_bytes(bias_s.at[0], d_send.at[0])
    wait_bytes(res_s.at[:, :, pl.ds(0, 1)], loc_sem.at[1])
    wait_bytes(res_s.at[:, :, pl.ds(0, rows - 1)], o_send.at[0])
    wait_bytes(res_s.at[:, :, pl.ds(0, rows - 1)], o_recv.at[0])


def solution(mesh):
    rows = mesh.shape['row']

    def body(pair_tile, res_mask, ln_gamma, ln_beta, w_q, w_k, w_v, w_b, w_g, w_o):
        block, width, chan = pair_tile.shape
        heads = w_b.shape[1]
        n = block * rows
        cols = width // rows
        bf16, f32 = jnp.bfloat16, jnp.float32
        nt = n // TILE
        sub = width // nt
        V = lambda *s, dt=bf16: pltpu.VMEM(s, dt)
        D = lambda *s: pltpu.SemaphoreType.DMA(s)
        out = pl.pallas_call(
            triangle_kernel,
            out_shape=pltpu.VMEM((width, 2, nt, sub, chan), bf16),
            in_specs=[pl.BlockSpec(memory_space=pl.ANY)] * 10,
            out_specs=pl.BlockSpec(memory_space=pltpu.VMEM),
            scratch_shapes=[V(block, width, chan), V(n, dt=jnp.int32), V(1, chan, dt=f32), V(1, chan, dt=f32), V(chan, chan), V(chan, chan),
                            V(chan, chan), V(heads, chan), V(chan, chan), V(chan, chan),
                            V(n, TILE, dt=f32), V(nt, block * sub, chan, dt=f32), V(block * sub, chan, dt=f32), V(width, 2, nt, sub, chan),
                            V(rows, cols, 2, nt, sub, chan), V(heads, sub, 128, dt=f32), V(2, nt, 2, sub, 128),
                            V(nt, rows, 2, sub, 128), V(2, nt, 2, RING, RING, 2, sub, n // 2), V(heads, n, TILE, dt=f32),
                            V(4, chan, chan), V(chan, heads * 128), V(cols, nt, chan, TILE, dt=f32), V(cols, heads, n, 128), V(cols, chan, n),
                            V(cols, nt, heads, 128, TILE), V(n, TILE, dt=f32), V(n, TILE, dt=f32), V(8, TILE, dt=f32), V(8, TILE, dt=f32),
                            V(cols, chan, TILE, dt=f32), V(nt, cols, rows, 2, sub, chan),
                            D(1), D(nt), D(1), D(cols // 2), D(2), D(nt, 2), D(nt, 2, RING), D(1), D(nt), D(1), D(1), D(2), D(nt), D(9)],
            compiler_params=pltpu.CompilerParams(vmem_limit_bytes=65_700_000, collective_id=0,
                                                 has_side_effects=True),
            name='triangle',
        )(pair_tile, res_mask, ln_gamma.reshape(1, chan), ln_beta.reshape(1, chan), w_q, w_k, w_v, w_b.T, w_g, w_o)
        return jnp.transpose(out.reshape(width, block, chan), (1, 0, 2))

    tile_spec = P(('data', 'row'), 'col', None)
    return jax.shard_map(body, mesh=mesh, in_specs=(tile_spec, P('data'), P(), P(), P(), P(), P(), P(), P(), P()), out_specs=tile_spec, check_vma=False)
```
